128 devices in a mesh: rep: 8 (over z, core), ep: 16 (over x, y).
Axes of the slice: x: 4, y: 4, z: 4, core: 2. Of those that a mesh axis runs over, the one named last changes fastest.
Arguments:
- latent_pages: bfloat16 [6144, 36864], P(('rep', 'ep')), may hold values from -4 to 4
- queries: bfloat16 [1024, 147456], P(('rep', 'ep')), may hold values from -4 to 4
- residual: bfloat16 [1024, 14336], P(('rep', 'ep')), may hold values from -6 to 6
- page_count: int32 [8, 16, 8], P(None, 'ep'), may hold values from 1 to 12, 48 in all within a row
- last_fill: int32 [8, 16, 8], P(None, 'ep'), may hold values from 4 to 64
- page_order: int32 [128, 48], P(('rep', 'ep')), may hold values from 0 to 47, each once within a row
- shed_slots: int32 [8, 16, 2], P(None, 'ep'), may hold values from 0 to 7, as said below
- shed_shift: int32 [16, 2], P('ep'), may hold values from 1 to 7
- expert_ids: int32 [4096, 8], P(('rep', 'ep')), may hold values from 0 to 127, all different within a row; in each aligned block of 32 rows (0 to 31, 32 to 63, ...) at most 4 rows name the same one
- gate_weight: float32 [4096, 8], P(('rep', 'ep')), may hold values from 0.05 to 0.5
- expert_home: int32 [128], replicated, may hold values from 0 to 127, each once
- norm_gain: float32 [3584], replicated, may hold values from 0.1 to 1.9
- value_up: bfloat16 [64, 512, 128], P('ep'), may hold values from -0.59765625 to 0.59765625
- out_weight: bfloat16 [8192, 3584], P('ep'), may hold values from -0.14941406 to 0.14941406
- expert_in: bfloat16 [128, 3584, 1024], P(('rep', 'ep')), may hold values from -0.09375 to 0.09375
- expert_out: bfloat16 [128, 1024, 3584], P(('rep', 'ep')), may hold values from -0.1875 to 0.1875
Outputs:
- attn_proj: bfloat16 [1024, 14336], P(('rep', 'ep'))
- layer_out: bfloat16 [1024, 14336], P(('rep', 'ep'))
The draws below stay inside these ranges and needn't reach their ends.
Inputs may be any that keep to these rules, and one draw needn't show every extreme that they name: `shed_slots`: for each device, 2 different slots. `expert_ids`: each row names 8 different experts; in the rows of one device no expert is named by more than 4 rows.
All inputs are finite; a program needn't handle non-finite values.
Results may differ from the reference program's by a relative error of at most 0.015.
Values may be sent and summed in bfloat16 or wider, within the bound.
No kernel may reach another device: no remote copies, remote signals or barrier semaphores. Data moves between devices by JAX's collectives and lax.ppermute only.
A program may use at most 192 MiB of HBM per device.

```python
import math
import jax
import jax.numpy as jnp
import numpy as np
from jax import lax

D = 3584
HEADS = 64
LAT = 512
KVW = 576
VHEAD = 128
FFE = 1024
TOP = 8
PAGE = 64
SPEC = 4
MAXP = 12
REQ_DEV = 8
SHED = 2
PAGES_DEV = 48
REQUESTS = 1024
TOK_DEV = 32
TOKENS = 4096
EXPERTS = 128
CAP = 4
N_REP = 8
N_EP = 16
DEVICES = 128


def draw_latent_pages(key, part):
    page_shape = (N_REP * N_EP * PAGES_DEV, PAGE, KVW)
    values = jnp.clip(jax.random.normal(key, page_shape, jnp.float32), -4.0, 4.0)
    return values.reshape(N_REP * N_EP * PAGES_DEV, PAGE * KVW).astype(jnp.bfloat16)


def draw_queries(key, part):
    ask_shape = (N_REP * N_EP * REQ_DEV, SPEC * HEADS, KVW)
    values = jnp.clip(jax.random.normal(key, ask_shape, jnp.float32), -4.0, 4.0)
    return values.reshape(N_REP * N_EP * REQ_DEV, SPEC * HEADS * KVW).astype(jnp.bfloat16)


def draw_shed_slots(key, part):
    split_keys = jax.random.split(jax.random.fold_in(key, 11), N_REP * N_EP)
    orders = jax.vmap(lambda single_key: jax.random.permutation(single_key, REQ_DEV))(split_keys)
    return orders[:, :SHED].reshape(N_REP, N_EP, SHED).astype(jnp.int32)


def with_ends(values, stream_key, least, largest):
    index_at = [jax.random.randint(jax.random.fold_in(stream_key, axis), (), 0, length) for axis, length in enumerate(values.shape)]
    longest = values.shape.index(max(values.shape))
    neighbour = index_at[:longest] + [(index_at[longest] + 1) % values.shape[longest]] + index_at[longest + 1:]
    return values.at[tuple(index_at)].set(least).at[tuple(neighbour)].set(largest)


def block_scale(stream_key, extent, pieces, least, largest):
    gain = 1.0
    for axis_at, parts in pieces:
        steps = jax.random.uniform(jax.random.fold_in(jax.random.fold_in(stream_key, 6), axis_at), (parts,), jnp.float32, least / len(pieces), largest / len(pieces))
        gain = gain * jnp.repeat(jnp.exp(steps), extent[axis_at] // parts).reshape((-1,) + (1,) * (len(extent) - 1 - axis_at))
    return gain


def profile(number_of, total, most, skew):
    portions = [(1 << 20) // math.isqrt(standing ** skew) + 1 for standing in range(2, number_of + 1)]
    spare, holding = total - most - (number_of - 1), [1] * (number_of - 1)
    while spare > 0:
        free = [i for i in range(number_of - 1) if holding[i] < most]
        whole, remaining = sum([portions[i] for i in free]), spare
        for i in free:
            more = min(most - holding[i], max(1, remaining * portions[i] // whole), spare)
            holding[i] = holding[i] + more
            spare = spare - more
    return np.array([most] + holding)


def uneven(stream_key, number_of, total, limit, lean):
    if number_of == 2:
        one = jax.random.randint(stream_key, (), max(1, total - limit), min(limit, total - 1) + 1)
        return jnp.stack([one, total - one])
    sizes = jnp.asarray(profile(number_of, total, limit, lean), jnp.int32)
    couples = (number_of - 1) // 2
    donor, sink = sizes[1:1 + 2 * couples:2], sizes[2:2 + 2 * couples:2]
    margin = jnp.minimum(donor - 1, limit - sink)
    moved = jax.random.randint(jax.random.fold_in(stream_key, 1), (couples,), 0, 1 << 20) % (margin + 1)
    sizes = sizes.at[1:1 + 2 * couples:2].set(donor - moved).at[2:2 + 2 * couples:2].set(sink + moved)
    return sizes[jax.random.permutation(jax.random.fold_in(stream_key, 2), number_of)]


def routed_block(key, own, number, rows, count, top, limit, skew):
    order = jax.random.permutation(key, count)
    heavy_load, usual = shares(count, rows * top, limit, skew, True), shares(count, rows * top, limit, skew, False)
    places = jnp.arange(count)

    def named(tallies, turn):
        used = int((tallies > 0).sum())
        fixed = max(1, used // 4)
        passed = fixed + (places - fixed + turn * (used - fixed)) % max(1, count - fixed)
        return jnp.zeros((count,), jnp.int32).at[order[jnp.where(places < fixed, places, passed)]].set(jnp.asarray(tallies, jnp.int32))

    tallies = jnp.where(number % 4 == 0, named(heavy_load, number // 4), named(usual, number - number // 4 - 1))
    mixed = jax.random.permutation(jax.random.fold_in(own, 3), count)
    source_of, receiver = mixed[0:count // 2 * 2:2], mixed[1:count // 2 * 2:2]
    slack = jnp.minimum(tallies[source_of] - 1, limit - tallies[receiver]) // 2
    slack = jnp.where((source_of == order[0]) | (receiver == order[0]) | (tallies[receiver] == 0), 0, jnp.maximum(slack, 0))
    passed = jax.random.randint(jax.random.fold_in(own, 4), (count // 2,), 0, 1 << 20) % (slack + 1)
    tallies = tallies.at[source_of].add(-passed).at[receiver].add(passed)
    items = jnp.searchsorted(jnp.cumsum(tallies), jnp.arange(rows * top), side="right").astype(jnp.int32)
    grid = items.reshape(top, rows).T
    grid = grid[jax.random.permutation(jax.random.fold_in(own, 1), rows)]
    turn = jax.random.randint(jax.random.fold_in(own, 2), (rows, 1), 0, top)
    return jnp.take_along_axis(grid, (jnp.arange(top)[None, :] + turn) % top, axis=1)


def shares(count, total, reach, skew, full):
    loads = [(1 << 20) // math.isqrt(standing ** skew) + 1 for standing in range(1, count + 1)]
    largest = reach if full else min(reach, max(-(-total // count), total * loads[0] // sum(loads)))
    least = 1 if total - largest >= count - 1 else 0
    holding, spare = [largest] + [least] * (count - 1), total - largest - least * (count - 1)
    while spare > 0:
        free = [i for i in range(1, count) if holding[i] < largest] or [i for i in range(1, count) if holding[i] < reach]
        pool, remaining = sum([loads[i] for i in free]), spare
        for i in free:
            extra = min(reach - holding[i], max(1, remaining * loads[i] // pool), spare)
            holding[i] = holding[i] + extra
            spare = spare - extra
    return np.array(holding)


def normal_values(key, extent, width, bound, shards=(), held_as=jnp.bfloat16):
    array = width * jax.random.normal(key, extent, jnp.float32)
    if shards:
        array = array * block_scale(key, extent, shards, -0.22, 0.18)
    return jnp.clip(array, -bound, bound).astype(held_as)


def setup_inputs(seed: int = 0) -> dict:
    splits = jax.random.split(jax.random.key(seed), 17)
    latent_pages = draw_latent_pages(jax.random.fold_in(splits[16], 71), 0)
    queries = draw_queries(jax.random.fold_in(splits[16], 71), 0)
    residual = normal_values(splits[2], (REQUESTS, SPEC * D), 1.0, 6.0, ((0, 128),))
    page_count = jax.vmap(lambda own: uneven(own, REQ_DEV, PAGES_DEV, MAXP, 2))(jax.random.split(splits[3], N_REP * N_EP)).reshape((N_REP, N_EP, REQ_DEV)).astype(jnp.int32)
    last_fill = with_ends(jax.random.randint(splits[4], (N_REP, N_EP, REQ_DEV), SPEC, PAGE + 1), jax.random.fold_in(splits[4], 1), SPEC, PAGE).astype(jnp.int32)
    page_order = jax.vmap(lambda own: jax.random.permutation(own, PAGES_DEV))(jax.random.split(splits[5], DEVICES)).reshape((DEVICES, PAGES_DEV)).astype(jnp.int32)
    shed_slots = draw_shed_slots(jax.random.fold_in(splits[16], 71), 0)
    shed_shift = with_ends(jax.random.randint(splits[7], (N_EP, SHED), 1, N_REP), jax.random.fold_in(splits[7], 1), 1, N_REP - 1).astype(jnp.int32)
    expert_ids_keys = jax.random.split(jax.random.fold_in(splits[8], 1), TOKENS // TOK_DEV)
    expert_ids_turns = jax.random.permutation(jax.random.fold_in(splits[8], 3), TOKENS // TOK_DEV)
    expert_ids = jax.vmap(lambda own, number: routed_block(jax.random.fold_in(splits[8], 2), own, number, TOK_DEV, EXPERTS, TOP, CAP, 2))(expert_ids_keys, expert_ids_turns).reshape((TOKENS, TOP))
    gate_weight = jnp.clip(0.05 + 0.45 * jax.random.uniform(splits[9], (TOKENS, TOP), jnp.float32) ** block_scale(splits[9], (TOKENS, TOP), ((0, 128),), -0.2, 0.2), 0.05, 0.5)
    expert_home = jax.random.permutation(splits[10], EXPERTS).astype(jnp.int32)
    norm_gain = jnp.clip(1.0 + 0.18 * jax.random.normal(splits[11], (D,), jnp.float32), 0.1, 1.9)
    value_up = normal_values(splits[12], (HEADS, LAT, VHEAD), 0.1, 0.59765625, ((0, 16),))
    out_weight = normal_values(splits[13], (HEADS * VHEAD, D), 0.025, 0.14941406, ((0, 16),))
    expert_in = normal_values(splits[14], (EXPERTS, D, FFE), D ** -0.5, 0.09375, ((0, 128),))
    expert_out = normal_values(splits[15], (EXPERTS, FFE, D), FFE ** -0.5, 0.1875, ((0, 128),))
    return dict(latent_pages=latent_pages, queries=queries, residual=residual, page_count=page_count, last_fill=last_fill, page_order=page_order, shed_slots=shed_slots, shed_shift=shed_shift, expert_ids=expert_ids, gate_weight=gate_weight, expert_home=expert_home, norm_gain=norm_gain, value_up=value_up, out_weight=out_weight, expert_in=expert_in, expert_out=expert_out)


SCORE_SCALE = 192.0 ** (-0.5)
NORM_EPS = 0.25

def serve_source(shed_slots, shed_shift):
    replicas = jnp.arange(N_REP, dtype=jnp.int32)[:, None, None]
    columns = jnp.arange(N_EP, dtype=jnp.int32)[None, :, None]
    shed_rank = jnp.arange(SHED, dtype=jnp.int32)[None, None, :]
    anchor_rep = ((replicas - shed_shift[None, :, :]) % N_REP).astype(jnp.int32)
    anchor_slot = shed_slots[anchor_rep, columns, shed_rank]
    anchor_id = ((anchor_rep * N_EP + columns) * REQ_DEV + anchor_slot).astype(jnp.int32)
    target_id = ((replicas * N_EP + columns) * REQ_DEV + shed_slots).astype(jnp.int32)
    identity = jnp.arange(N_REP * N_EP * REQ_DEV, dtype=jnp.int32)
    return identity.at[target_id.reshape(-1)].set(anchor_id.reshape(-1))

def page_tables(page_count, page_order):
    counts_flat = page_count.reshape(N_REP * N_EP, REQ_DEV).astype(jnp.int32)
    offsets = (jnp.cumsum(counts_flat, axis=1) - counts_flat).astype(jnp.int32)
    page_steps = jnp.arange(MAXP, dtype=jnp.int32)
    positions = jnp.minimum(offsets[:, :, None] + page_steps[None, None, :], PAGES_DEV - 1).astype(jnp.int32)
    local_rows = jax.vmap(lambda order_row, spot_list: order_row[spot_list])(page_order, positions)
    base_rows = (jnp.arange(N_REP * N_EP, dtype=jnp.int32) * PAGES_DEV)[:, None, None]
    return (local_rows + base_rows).reshape(N_REP * N_EP * REQ_DEV, MAXP).astype(jnp.int32)

def attend_rows(key_rows, query_rows, length):
    scores = jnp.dot(query_rows, key_rows.T, preferred_element_type=jnp.float32) * SCORE_SCALE
    position = jnp.arange(MAXP * PAGE, dtype=jnp.int32)
    offset = jnp.arange(SPEC * HEADS, dtype=jnp.int32) // HEADS
    visible_end = length - SPEC + 1 + offset
    visible = position[None, :] < visible_end[:, None]
    scores = jnp.where(visible, scores, -1e+30)
    exponent = jnp.exp(scores - lax.optimization_barrier(jnp.max(scores, axis=1, keepdims=True)))
    probability = (exponent / lax.optimization_barrier(jnp.sum(exponent, axis=1, keepdims=True))).astype(jnp.bfloat16)
    return jnp.dot(probability, key_rows[:, :LAT], preferred_element_type=jnp.float32).astype(jnp.bfloat16)

def reference(latent_pages, queries, residual, page_count, last_fill, page_order, shed_slots, shed_shift, expert_ids, gate_weight, expert_home, norm_gain, value_up, out_weight, expert_in, expert_out):
    requests = N_REP * N_EP * REQ_DEV
    tokens = requests * SPEC
    source = serve_source(shed_slots, shed_shift)
    tables = page_tables(page_count, page_order)
    lengths = ((page_count - 1) * PAGE + last_fill).reshape(requests).astype(jnp.int32)

    def attend_slot(serving):
        anchor = source[serving]
        key_rows = latent_pages[tables[anchor]].reshape(MAXP * PAGE, KVW)
        query_rows = queries[anchor].reshape(SPEC * HEADS, KVW)
        return attend_rows(key_rows, query_rows, lengths[anchor])
    latent_out = lax.map(attend_slot, jnp.arange(requests, dtype=jnp.int32))
    replica_blocks = latent_out.reshape(N_REP, N_EP * REQ_DEV * SPEC, HEADS, LAT)

    def project(replica_rows):
        lifted = jnp.einsum('thl,hlv->thv', replica_rows.astype(jnp.float32), value_up.astype(jnp.float32)).astype(jnp.bfloat16)
        return jnp.dot(lifted.reshape(replica_rows.shape[0], HEADS * VHEAD), out_weight, preferred_element_type=jnp.float32)
    branch = lax.map(project, replica_blocks).reshape(tokens, D)
    mixed = residual[source].reshape(tokens, D).astype(jnp.float32) + branch
    square = lax.optimization_barrier(jnp.mean(mixed * mixed, axis=1, keepdims=True))
    normed = (mixed * lax.rsqrt(square + NORM_EPS) * norm_gain).astype(jnp.bfloat16)
    flat_ids = expert_ids.reshape(-1)
    flat_gates = gate_weight.reshape(-1)
    most_rows = N_REP * N_EP * CAP

    def expert_step(running, expert):
        chosen = flat_ids == expert
        found_at = jnp.nonzero(chosen, size=most_rows, fill_value=0)[0].astype(jnp.int32)
        filled = jnp.arange(most_rows) < jnp.sum(chosen)
        owners = (found_at // TOP).astype(jnp.int32)
        weights = jnp.where(filled, flat_gates[found_at], 0.0)
        placed = expert_home[expert]
        inner_act = jax.nn.silu(jnp.dot(normed[owners], expert_in[placed], preferred_element_type=jnp.float32)).astype(jnp.bfloat16)
        outer_out = jnp.dot(inner_act, expert_out[placed], preferred_element_type=jnp.float32).astype(jnp.bfloat16)
        return (running.at[owners].add(weights[:, None] * outer_out.astype(running.dtype)), None)
    moe_sum, unused = lax.scan(expert_step, jnp.zeros((tokens, D), jnp.float32), jnp.arange(EXPERTS, dtype=jnp.int32))
    attn_proj = branch.astype(jnp.bfloat16).reshape(requests, SPEC * D)
    layer_out = (mixed + moe_sum).astype(jnp.bfloat16).reshape(requests, SPEC * D)
    return (attn_proj, layer_out)
```

```python
import jax
import jax.numpy as jnp
from jax import lax
from jax.sharding import Mesh
from jax.sharding import PartitionSpec as P

D = 3584
HEADS = 64
LAT = 512
KVW = 576
VHEAD = 128
TOP = 8
PAGE = 64
SPEC = 4
MAXP = 12
REQ_DEV = 8
PAGES_DEV = 48
EP = ("ep_0", "ep_1")
REP_EP = ("rep", "ep_0", "ep_1")


SCORE_SCALE = 192.0 ** (-0.5)
NORM_EPS = 0.25


def shifted(value, axis, steps):
    count = lax.axis_size(axis)
    pairs = [(source, (source + steps) % count) for source in range(count)]
    return lax.ppermute(value, axis, pairs)


def own_rows_2(terms, axes):
    so_far = terms.astype(jnp.bfloat16)
    for axis in axes:
        so_far = lax.psum_scatter(so_far, axis, scatter_dimension=0, tiled=True)
    return so_far.astype(jnp.float32)


def attend(key_block, query_block, lengths):
    request_count = key_block.shape[0]
    key_rows = key_block.reshape(request_count, MAXP * PAGE, KVW)
    query_rows = query_block.reshape(request_count, SPEC * HEADS, KVW)
    scores = (
        jnp.einsum("rqc,rkc->rqk", query_rows, key_rows, preferred_element_type=jnp.float32)
        * SCORE_SCALE
    )
    position = jnp.arange(MAXP * PAGE, dtype=jnp.int32)
    offset = jnp.arange(SPEC * HEADS, dtype=jnp.int32) // HEADS
    visible_end = lengths[:, None] - SPEC + 1 + offset[None, :]
    visible = position[None, None, :] < visible_end[:, :, None]
    scores = jnp.where(visible, scores, -1e30)
    exponent = jnp.exp(scores - jnp.max(scores, axis=2, keepdims=True))
    probability = (exponent / jnp.sum(exponent, axis=2, keepdims=True)).astype(jnp.bfloat16)
    latent = jnp.einsum(
        "rqk,rkl->rql", probability, key_rows[:, :, :LAT], preferred_element_type=jnp.float32
    )
    return latent.astype(jnp.bfloat16).reshape(request_count, SPEC * HEADS * LAT)


def fill_slots(arrived, picker, present, own_rows):
    return jnp.where(present[:, None], arrived[picker], own_rows)


def per_device(
    latent_pages,
    queries,
    residual,
    page_count,
    last_fill,
    page_order,
    shed_slots,
    shed_shift,
    expert_ids,
    gate_weight,
    expert_home,
    norm_gain,
    value_up,
    out_weight,
    expert_in,
    expert_out,
):
    rep_count = lax.axis_size("rep")
    col_count = lax.axis_size(EP)
    device_count = rep_count * col_count
    replica = lax.axis_index("rep")
    lengths = (page_count[:, 0, :] - 1) * PAGE + last_fill[:, 0, :]
    shed_table = shed_slots[:, 0, :]
    own_counts = page_count[replica, 0, :]
    offsets = jnp.cumsum(own_counts) - own_counts
    page_steps = jnp.arange(MAXP, dtype=jnp.int32)
    positions = jnp.minimum(offsets[:, None] + page_steps[None, :], PAGES_DEV - 1)
    own_keys = latent_pages[page_order[0][positions]].reshape(REQ_DEV, MAXP * PAGE * KVW)
    own_lengths = lengths[replica]
    own_sheds = shed_table[replica]
    shifts = shed_shift[0]
    matches = own_sheds[None, :] == jnp.arange(REQ_DEV, dtype=jnp.int32)[:, None]
    present = jnp.any(matches, axis=1)
    picker = jnp.argmax(matches, axis=1)
    own_latent = attend(own_keys, queries, own_lengths)
    tokens_dev = REQ_DEV * SPEC
    heads_dev = value_up.shape[0]
    token_latent = own_latent.reshape(tokens_dev, HEADS * LAT)
    regrouped = lax.all_to_all(token_latent, EP, split_axis=1, concat_axis=0, tiled=True)
    row_block = regrouped.reshape(tokens_dev * lax.axis_size(EP), heads_dev, LAT)
    lifted = jnp.einsum(
        "thl,hlv->thv", row_block, value_up, preferred_element_type=jnp.float32
    ).astype(jnp.bfloat16)
    branch = own_rows_2(
        jnp.dot(
            lifted.reshape(tokens_dev * lax.axis_size(EP), heads_dev * VHEAD),
            out_weight,
            preferred_element_type=jnp.float32,
        ),
        EP,
    )
    own_branch = branch.astype(jnp.bfloat16).reshape(REQ_DEV, SPEC * D)
    arrived = jnp.concatenate((own_branch[own_sheds], residual[own_sheds]), axis=1)
    for bit_level in range(rep_count.bit_length() - 1):
        moved = shifted(arrived, "rep", 1 << bit_level)
        taking = shifts // (1 << bit_level) % 2 == 1
        arrived = jnp.where(taking[:, None], moved, arrived)
    served_branch = fill_slots(arrived[:, : SPEC * D], picker, present, own_branch)
    served_rest = fill_slots(arrived[:, SPEC * D :], picker, present, residual)
    branch = served_branch.reshape(tokens_dev, D).astype(jnp.float32)
    mixed = served_rest.reshape(tokens_dev, D).astype(jnp.float32) + branch
    square = jnp.mean(mixed * mixed, axis=1, keepdims=True)
    normed = (mixed * lax.rsqrt(square + NORM_EPS) * norm_gain).astype(jnp.bfloat16)
    capacity = max(4, 2 * tokens_dev * TOP // device_count)
    flat_ids = expert_ids.reshape(-1)
    target = expert_home[flat_ids]
    hits = (target[:, None] == jnp.arange(device_count, dtype=jnp.int32)[None, :]).astype(jnp.int32)
    before = jnp.sum((jnp.cumsum(hits, axis=0) - hits) * hits, axis=1)
    slot_index = target * capacity + before
    buffer_rows = jnp.arange(device_count * capacity, dtype=jnp.int32)
    landing = buffer_rows[:, None, None] == slot_index.reshape(tokens_dev, TOP)[None, :, :]
    chooser = jnp.any(landing, axis=2).astype(jnp.bfloat16)
    outgoing_tokens = jnp.dot(chooser, normed, preferred_element_type=jnp.float32).astype(
        jnp.bfloat16
    )
    incoming = lax.all_to_all(
        outgoing_tokens.reshape(device_count, capacity, D),
        REP_EP,
        split_axis=0,
        concat_axis=0,
        tiled=True,
    )
    inner_act = jax.nn.silu(
        jnp.dot(
            incoming.reshape(device_count * capacity, D),
            expert_in[0],
            preferred_element_type=jnp.float32,
        )
    ).astype(jnp.bfloat16)
    outer_out = jnp.dot(inner_act, expert_out[0], preferred_element_type=jnp.float32).astype(
        jnp.bfloat16
    )
    returned = lax.all_to_all(
        outer_out.reshape(device_count, capacity, D),
        REP_EP,
        split_axis=0,
        concat_axis=0,
        tiled=True,
    )
    picked = (
        returned.reshape(device_count * capacity, D)[slot_index]
        .reshape(tokens_dev, TOP, D)
        .astype(jnp.float32)
    )
    moe_sum = jnp.sum(gate_weight[:, :, None] * picked, axis=1)
    attn_proj = served_branch
    layer_out = (mixed + moe_sum).astype(jnp.bfloat16).reshape(REQ_DEV, SPEC * D)
    return (attn_proj, layer_out)


def solution(mesh):
    torus = Mesh(mesh.devices.reshape(mesh.shape["rep"], 4, 4), ("rep", "ep_0", "ep_1"))
    return jax.shard_map(
        per_device,
        mesh=torus,
        in_specs=(
            P(REP_EP, None),
            P(REP_EP, None),
            P(REP_EP, None),
            P(None, EP, None),
            P(None, EP, None),
            P(REP_EP, None),
            P(None, EP, None),
            P(EP, None),
            P(REP_EP, None),
            P(REP_EP, None),
            P(),
            P(),
            P(EP, None, None),
            P(EP, None),
            P(REP_EP, None, None),
            P(REP_EP, None, None),
        ),
        out_specs=(P(REP_EP, None), P(REP_EP, None)),
        check_vma=False,
    )
```

```python
import jax
import jax.numpy as jnp
from jax import lax
from jax.experimental import pallas as pl
from jax.experimental.pallas import tpu as pltpu
from jax.sharding import Mesh
from jax.sharding import PartitionSpec as P

D = 3584
HALF = D // 2
HEADS = 64
LAT = 512
KVW = 576
VHEAD = 128
FFE = 1024
TOP = 8
PAGE = 64
SPEC = 4
MAXP = 12
REQ_DEV = 8
PAGES_DEV = 48
TOK_DEV = REQ_DEV * SPEC
N_EP = 16
HEADS_DEV = HEADS // N_EP
DEVICES = 128
CAP = 4
BAND = D // 4
KEYS = MAXP * PAGE
EP = ("ep_0", "ep_1")
REP_EP = ("rep", "ep_0", "ep_1")
SCORE_SCALE = 192.0 ** (-0.5)
NORM_EPS = 0.25
BF = jnp.bfloat16
F32 = jnp.float32


def iota2(rows, cols, dim):
    return lax.broadcasted_iota(jnp.int32, (rows, cols), dim)


def rows_first(source_of, size=256):
    return (iota2(size, size, 1) == source_of(iota2(size, size, 0))).astype(BF)


def mm(a, b):
    return jnp.dot(a, b, preferred_element_type=F32)


def attention_body(page_ids, lengths, query_ref, page_ref, out_ref, key_ref):
    request = pl.program_id(0)

    def bring(step, carry):
        start = pl.multiple_of(step * PAGE, PAGE)
        key_ref[pl.ds(start, PAGE), :] = page_ref[page_ids[request * MAXP + step]]
        return carry

    lax.fori_loop(0, MAXP, bring, 0)
    scores = lax.dot_general(
        query_ref[0], key_ref[...], (((1,), (1,)), ((), ())), preferred_element_type=F32
    )
    rows = SPEC * HEADS
    visible_end = lengths[request] - SPEC + 1 + iota2(rows, KEYS, 0) // HEADS
    scores = jnp.where(iota2(rows, KEYS, 1) < visible_end, scores * SCORE_SCALE, -1e30)
    exponent = jnp.exp(scores - jnp.max(scores, axis=1, keepdims=True))
    total = jnp.sum(exponent, axis=1, keepdims=True)
    latent = mm(exponent.astype(BF), key_ref[:, :LAT]) / total
    order = rows_first(lambda r: (r // 4 % 4) * 64 + (r // 16) * 4 + r % 4)
    out_ref[...] = mm(order, latent.astype(BF)).astype(BF).reshape(N_EP, 16, LAT)


def attention(page_ids, lengths, query_rows, pages):
    return pl.pallas_call(
        attention_body,
        grid_spec=pltpu.PrefetchScalarGridSpec(
            num_scalar_prefetch=2,
            grid=(REQ_DEV,),
            in_specs=[
                pl.BlockSpec((1, SPEC * HEADS, KVW), lambda i, *_: (i, 0, 0)),
                pl.BlockSpec((PAGES_DEV, PAGE, KVW), lambda i, *_: (0, 0, 0)),
            ],
            out_specs=pl.BlockSpec((N_EP, 16, LAT), lambda i, *_: (0, i, 0)),
            scratch_shapes=[pltpu.VMEM((KEYS, KVW), BF)],
        ),
        out_shape=jax.ShapeDtypeStruct((N_EP, REQ_DEV * 16, LAT), BF),
        cost_estimate=pl.CostEstimate(
            flops=8 * 256 * 768 * 1088 * 2, bytes_accessed=10 << 20, transcendentals=8 * 256 * 768
        ),
        name="attention",
    )(page_ids, lengths, query_rows, pages)


def project_body(order_ref, latent_ref, up_ref, weight_ref, *rest):
    outs, (split_ref, lifted_ref, picked_ref) = rest[:8], rest[8:]
    by_head = rows_first(lambda r: (r % 64) * 4 + r // 64)

    def split(step, carry):
        both = mm(by_head, latent_ref[step]).astype(BF)
        for head in range(HEADS_DEV):
            split_ref[head, pl.ds(pl.multiple_of(step * 64, 64), 64), :] = both[
                head * 64 : head * 64 + 64
            ]
        return carry

    lax.fori_loop(0, 8, split, 0)
    for head in range(HEADS_DEV):
        lifted = mm(split_ref[head], up_ref[head]).astype(BF)
        lifted_ref[:, :, head * VHEAD : (head + 1) * VHEAD] = lifted.reshape(N_EP, 32, VHEAD)
    for band in range(4):
        for place in range(N_EP):
            picked_ref[place * 32 : place * 32 + 32, :] = lifted_ref[order_ref[band * N_EP + place]]
        part = mm(picked_ref[...], weight_ref[:, band * BAND : (band + 1) * BAND]).astype(BF)
        outs[2 * band][...] = part[:256]
        outs[2 * band + 1][...] = part[256:]


def project(order, latent, value_up, out_weight):
    whole = pl.BlockSpec(memory_space=pltpu.VMEM)
    return pl.pallas_call(
        project_body,
        in_specs=[pl.BlockSpec(memory_space=pltpu.SMEM), whole, whole, whole],
        out_specs=[whole] * 8,
        out_shape=[jax.ShapeDtypeStruct((256, BAND), BF)] * 8,
        scratch_shapes=[
            pltpu.VMEM((HEADS_DEV, 512, LAT), BF),
            pltpu.VMEM((N_EP, 32, 512), BF),
            pltpu.VMEM((512, 512), BF),
        ],
        cost_estimate=pl.CostEstimate(
            flops=3 << 30, bytes_accessed=10 << 20, transcendentals=0
        ),
        name="project",
    )(order, latent, value_up, out_weight)


def expert_body(x_ref, in_hbm, out_hbm, o_ref, x_s, h_s, in_s, out_s, in_sem, out_sem):
    def in_copy(j):
        return pltpu.make_async_copy(
            in_hbm.at[0, :, pl.ds(pl.multiple_of(j * 256, 256), 256)], in_s.at[j], in_sem.at[j]
        )

    def out_copy(j, half):
        at = pl.multiple_of(half * HALF + j * 256, 256)
        return pltpu.make_async_copy(
            out_hbm.at[0, :, pl.ds(at, 256)], out_s.at[j, half], out_sem.at[j, half]
        )

    for j in range(4):
        in_copy(j).start()
    for j in range(7):
        out_copy(j, 0).start()
        out_copy(j, 1).start()
    apart = rows_first(lambda r: (r % 128 // 4) * 8 + (r // 128) * 4 + r % 4)
    joined = rows_first(lambda r: (r // 4 % 2) * 128 + (r // 8) * 4 + r % 4)

    def part(step, carry):
        block = x_ref[pl.ds(pl.multiple_of(step * 256, 256), 256), :]
        block = mm(apart, block).astype(BF)
        at = pl.multiple_of(step * 128, 128)
        x_s[0, pl.ds(at, 128), :] = block[:128]
        x_s[1, pl.ds(at, 128), :] = block[128:]
        return carry

    lax.fori_loop(0, 4, part, 0)

    def inner(j, carry):
        in_copy(j).wait()
        value = mm(x_s[0], in_s[j, :HALF]) + mm(x_s[1], in_s[j, HALF:])
        h_s[j] = (value / (1.0 + jnp.exp(-value))).astype(BF)
        return carry

    lax.fori_loop(0, 4, inner, 0)

    def outer(j, carry):
        halves = []
        for half in range(2):
            out_copy(j, half).wait()
            total = mm(h_s[0], out_s[j, half, :256])
            for k in range(1, 4):
                total += mm(h_s[k], out_s[j, half, k * 256 : (k + 1) * 256])
            halves.append(total.astype(BF))
        at = pl.multiple_of(j * 256, 256)
        for step in range(4):
            rows = slice(step * 128, step * 128 + 128)
            both = jnp.concatenate((halves[0][rows], halves[1][rows]), axis=0)
            o_ref[step * 256 : step * 256 + 256, pl.ds(at, 256)] = mm(joined, both).astype(BF)
        return carry

    lax.fori_loop(0, 7, outer, 0)


def expert(incoming, expert_in, expert_out):
    whole = pl.BlockSpec(memory_space=pltpu.VMEM)
    far = pl.BlockSpec(memory_space=pl.ANY)
    return pl.pallas_call(
        expert_body,
        in_specs=[whole, far, far],
        out_specs=whole,
        out_shape=jax.ShapeDtypeStruct((DEVICES * 8, HALF), BF),
        scratch_shapes=[
            pltpu.VMEM((2, 512, HALF), BF),
            pltpu.VMEM((4, 512, 256), BF),
            pltpu.VMEM((4, D, 256), BF),
            pltpu.VMEM((7, 2, FFE, 256), BF),
            pltpu.SemaphoreType.DMA((4,)),
            pltpu.SemaphoreType.DMA((7, 2)),
        ],
        cost_estimate=pl.CostEstimate(
            flops=8 << 30, bytes_accessed=22 << 20, transcendentals=512 * 1024
        ),
        name="expert",
    )(incoming, expert_in, expert_out)


NEAR = [(0, 1), (1, 0), (2, 3), (3, 2)]
FAR = [(0, 3), (3, 0), (1, 2), (2, 1)]
PAIRS = {1: NEAR, 3: FAR}
ROUTES = (
    (("ep_0", 1), ("ep_0", 3), ("ep_1", 1), ("ep_1", 3)),
    (("ep_0", 3), ("ep_0", 1), ("ep_1", 3), ("ep_1", 1)),
    (("ep_1", 1), ("ep_1", 3), ("ep_0", 1), ("ep_0", 3)),
    (("ep_1", 3), ("ep_1", 1), ("ep_0", 3), ("ep_0", 1)),
)


def block_order():
    first, second = [], []
    for route in ROUTES:
        places = [(0, 0)]
        for axis, flip in reversed(route):
            turn = (flip, 0) if axis == "ep_0" else (0, flip)
            places = places + [(a ^ turn[0], b ^ turn[1]) for a, b in places]
        first += [a for a, _ in places]
        second += [b for _, b in places]
    mine = lax.axis_index("ep_0"), lax.axis_index("ep_1")
    return (jnp.array(first, jnp.int32) ^ mine[0]) * 4 + (jnp.array(second, jnp.int32) ^ mine[1])


def sum_over_columns(parts):
    kept = [parts[2 * band] for band in range(4)]
    sent = [parts[2 * band + 1] for band in range(4)]
    arrived = [[] for _ in range(4)]
    rows = 256
    for step in range(4):
        for band in range(4):
            axis, flip = ROUTES[band][step]
            arrived[band].append(lax.ppermute(sent[band], axis, PAIRS[flip]))
        if step == 3:
            break
        rows //= 2
        for band in range(4):
            total = kept[band][rows : 2 * rows].astype(F32)
            for piece in arrived[band]:
                total = total + piece[rows : 2 * rows].astype(F32)
            sent[band] = total.astype(BF)
    sums = []
    for band in range(4):
        total = kept[band][:rows].astype(F32)
        for piece in arrived[band]:
            total = total + piece[:rows].astype(F32)
        sums.append(total)
    return jnp.concatenate(sums, axis=1)


def shifted(value, axis, steps):
    count = lax.axis_size(axis)
    return lax.ppermute(value, axis, [(s, (s + steps) % count) for s in range(count)])


def ship(value, shifts):
    for bit in range(3):
        moved = shifted(value, "rep", 1 << bit)
        value = jnp.where((shifts // (1 << bit) % 2 == 1)[:, None], moved, value)
    return value


def per_device(
    latent_pages,
    queries,
    residual,
    page_count,
    last_fill,
    page_order,
    shed_slots,
    shed_shift,
    expert_ids,
    gate_weight,
    expert_home,
    norm_gain,
    value_up,
    out_weight,
    expert_in,
    expert_out,
):
    replica = lax.axis_index("rep")
    own_counts = page_count[replica, 0, :]
    own_lengths = (own_counts - 1) * PAGE + last_fill[replica, 0, :]
    offsets = jnp.cumsum(own_counts) - own_counts
    steps = jnp.arange(MAXP, dtype=jnp.int32)
    positions = jnp.minimum(offsets[:, None] + steps[None, :], PAGES_DEV - 1)
    page_ids = page_order[0][positions].reshape(-1)

    latent = attention(
        page_ids,
        own_lengths,
        queries.reshape(REQ_DEV, SPEC * HEADS, KVW),
        latent_pages.reshape(PAGES_DEV, PAGE, KVW),
    )
    gathered = lax.all_to_all(latent, EP, split_axis=0, concat_axis=0, tiled=True)
    parts = project(block_order(), gathered.reshape(8, 256, LAT), value_up, out_weight)
    own_branch = sum_over_columns(parts).astype(BF)

    tokens = jnp.arange(TOK_DEV, dtype=jnp.int32)
    own_sheds = shed_slots[replica, 0, :]
    shed_rows = (own_sheds[:, None] * SPEC + jnp.arange(SPEC, dtype=jnp.int32)).reshape(-1)
    pick = shed_rows[:, None] == tokens[None, :]
    present = jnp.any(pick, axis=0)[:, None]
    pick = pick.astype(BF)
    row_shifts = jnp.repeat(shed_shift[0], SPEC)
    own_residual = residual.reshape(TOK_DEV, D)

    def serve(own):
        came = ship(mm(pick, own).astype(BF), row_shifts)
        return jnp.where(present, mm(pick.T, came).astype(BF), own)

    served_residual = serve(own_residual)
    served_branch = serve(own_branch)
    mixed = served_residual.astype(F32) + served_branch.astype(F32)
    square = jnp.mean(mixed * mixed, axis=1, keepdims=True)
    normed = (mixed * lax.rsqrt(square + NORM_EPS) * norm_gain).astype(BF)

    target = expert_home[expert_ids.reshape(-1)]
    hits = (target[:, None] == jnp.arange(DEVICES, dtype=jnp.int32)[None, :]).astype(jnp.int32)
    before = jnp.sum((jnp.cumsum(hits, axis=0) - hits) * hits, axis=1)
    slot = (target * CAP + before).reshape(TOK_DEV, TOP)
    row = jnp.arange(DEVICES * 8, dtype=jnp.int32)
    row_slot = row // 8 * CAP + row % CAP
    row_half = row // CAP % 2
    both = jnp.arange(2 * TOK_DEV, dtype=jnp.int32)
    same_half = row_half[None, :] == (both // TOK_DEV)[:, None]
    landing = slot[:, :, None] == row_slot[None, None, :]
    chosen = jnp.any(landing, axis=1)
    chooser = (jnp.concatenate((chosen, chosen)) & same_half).astype(BF)
    gates = jnp.sum(jnp.where(landing, gate_weight[:, :, None], 0.0), axis=1)
    gates = jnp.where(same_half, jnp.concatenate((gates, gates)), 0.0)
    coarse = lax.reduce_precision(gates, 8, 7)
    gates = jnp.concatenate((coarse.astype(BF), (gates - coarse).astype(BF)))

    def halves(value):
        return jnp.concatenate((value[:, :HALF], value[:, HALF:]), axis=0)

    outgoing = lax.dot_general(
        chooser, halves(normed), (((0,), (0,)), ((), ())), preferred_element_type=F32
    ).astype(BF)
    incoming = lax.all_to_all(outgoing, REP_EP, split_axis=0, concat_axis=0, tiled=True)
    outer = expert(incoming, expert_in, expert_out)
    returned = lax.all_to_all(outer, REP_EP, split_axis=0, concat_axis=0, tiled=True)
    moe = mm(gates, returned)
    layer = (halves(mixed) + moe[: 2 * TOK_DEV] + moe[2 * TOK_DEV :]).astype(BF)
    layer_out = jnp.concatenate((layer[:TOK_DEV], layer[TOK_DEV:]), axis=1)
    return (
        served_branch.reshape(REQ_DEV, SPEC * D),
        layer_out.reshape(REQ_DEV, SPEC * D),
    )


def solution(mesh):
    torus = Mesh(mesh.devices.reshape(mesh.shape["rep"], 4, 4), ("rep", "ep_0", "ep_1"))
    return jax.shard_map(
        per_device,
        mesh=torus,
        in_specs=(
            P(REP_EP, None),
            P(REP_EP, None),
            P(REP_EP, None),
            P(None, EP, None),
            P(None, EP, None),
            P(REP_EP, None),
            P(None, EP, None),
            P(EP, None),
            P(REP_EP, None),
            P(REP_EP, None),
            P(),
            P(),
            P(EP, None, None),
            P(EP, None),
            P(REP_EP, None, None),
            P(REP_EP, None, None),
        ),
        out_specs=(P(REP_EP, None), P(REP_EP, None)),
        check_vma=False,
    )
```

```python
import jax
import jax.numpy as jnp
from jax import lax
from jax.experimental import pallas as pl
from jax.experimental.pallas import tpu as pltpu
from jax.sharding import Mesh
from jax.sharding import PartitionSpec as P

D = 3584
HALF = D // 2
HEADS = 64
LAT = 512
KVW = 576
VHEAD = 128
FFE = 1024
TOP = 8
PAGE = 64
SPEC = 4
MAXP = 12
REQ_DEV = 8
PAGES_DEV = 48
TOK_DEV = REQ_DEV * SPEC
N_EP = 16
HEADS_DEV = HEADS // N_EP
DEVICES = 128
CAP = 4
BAND = D // 4
KEYS = MAXP * PAGE
EP = ("ep_0", "ep_1")
REP_EP = ("rep", "ep_0", "ep_1")
SCORE_SCALE = 192.0 ** (-0.5)
NORM_EPS = 0.25
BF = jnp.bfloat16
F32 = jnp.float32


def iota2(rows, cols, dim):
    return lax.broadcasted_iota(jnp.int32, (rows, cols), dim)


def rows_first(source_of, size=256):
    return (iota2(size, size, 1) == source_of(iota2(size, size, 0))).astype(BF)


def mm(a, b):
    return jnp.dot(a, b, preferred_element_type=F32)


def near(value):
    return pltpu.with_memory_space_constraint(value, pltpu.VMEM)


def distant(value):
    return pltpu.with_memory_space_constraint(value, pltpu.HBM)


WINDOW = 12


def attention_body(starts, skips, lengths, order_ref, query_ref, page_ref, out_ref, key_s, piece_s, query_s):
    to_place = (iota2(384, 384, 1) == order_ref[...]).astype(BF)
    for group in range(8):
        tokens = [
            page_ref[:, (group * 8 + t) * KVW : (group * 8 + t + 1) * KVW] for t in range(8)
        ]
        key_s[group] = mm(to_place, jnp.concatenate(tokens, axis=0))
    by_request = rows_first(lambda r: (r % 32) * 8 + r // 32)
    for pair in range(8):
        for column in range(2):
            for position in range(SPEC):
                for head in range(HEADS_DEV):
                    at = position * HEADS + (pair * 2 + column) * HEADS_DEV + head
                    place = (column * SPEC + position) * HEADS_DEV + head
                    piece_s[place * 8 : place * 8 + 8, :] = query_ref[
                        :, at * KVW : (at + 1) * KVW
                    ].astype(F32)
        rows = mm(by_request, piece_s[...].astype(BF)).astype(BF)
        query_s[:, pair * 32 : pair * 32 + 32, :] = rows.reshape(REQ_DEV, 32, KVW)

    def request(i, carry):
        start = pl.multiple_of(starts[i] * 8, 8)
        keys = key_s[:, pl.ds(start, WINDOW * 8), :].reshape(KEYS, KVW).astype(BF)
        scores = lax.dot_general(
            query_s[i], keys, (((1,), (1,)), ((), ())), preferred_element_type=F32
        )
        rows = SPEC * HEADS
        visible_end = lengths[i] - SPEC + 1 + iota2(rows, 1, 0) // HEADS_DEV % SPEC
        key = iota2(1, KEYS, 1)
        page = key % (WINDOW * 8) // 8 - skips[i]
        token = page * PAGE + key // (WINDOW * 8) * 8 + key % 8
        token = jnp.where(page < 0, KEYS, token)
        scores = jnp.where(token < visible_end, scores * SCORE_SCALE, -1e30)
        exponent = jnp.exp(scores - jnp.max(scores, axis=1, keepdims=True))
        total = jnp.sum(exponent, axis=1, keepdims=True)
        latent = mm(exponent.astype(BF), keys[:, :LAT]) / total
        out_ref[:, pl.ds(pl.multiple_of(i * 16, 16), 16), :] = latent.astype(BF).reshape(
            N_EP, 16, LAT
        )
        return carry

    lax.fori_loop(0, REQ_DEV, request, 0)


def attention(page_order, offsets, lengths, queries, pages):
    starts = jnp.minimum(offsets, PAGES_DEV - WINDOW)
    row = jnp.arange(PAGES_DEV * 8, dtype=jnp.int32)
    order = (jnp.repeat(page_order, 8) + row % 8 * PAGES_DEV)[:, None]
    whole = pl.BlockSpec(memory_space=pltpu.VMEM)
    few = pl.BlockSpec(memory_space=pltpu.SMEM)
    return pl.pallas_call(
        attention_body,
        in_specs=[few, few, few, whole, whole, whole],
        out_specs=whole,
        out_shape=jax.ShapeDtypeStruct((N_EP, REQ_DEV * 16, LAT), BF),
        scratch_shapes=[
            pltpu.VMEM((8, PAGES_DEV * 8, KVW), F32),
            pltpu.VMEM((256, KVW), F32),
            pltpu.VMEM((REQ_DEV, SPEC * HEADS, KVW), BF),
        ],
        cost_estimate=pl.CostEstimate(
            flops=8 * 256 * 768 * 1088 * 2, bytes_accessed=10 << 20, transcendentals=8 * 256 * 768
        ),
        compiler_params=pltpu.CompilerParams(vmem_limit_bytes=36 << 20),
        name="attention",
    )(starts, offsets - starts, lengths, order, near(queries), near(pages))


def project_body(order_ref, latent_ref, up_hbm, weight_hbm, *rest):
    outs = rest[:8]
    split_ref, lifted_ref, picked_ref, part_ref, up_ref, weight_ref, in_sems, sems = rest[8:]
    loads = [pltpu.make_async_copy(up_hbm, up_ref, in_sems.at[4])]
    for band in range(4):
        columns = pl.ds(band * BAND, BAND)
        loads.append(
            pltpu.make_async_copy(
                weight_hbm.at[:, columns], weight_ref.at[:, columns], in_sems.at[band]
            )
        )
    for load in loads:
        load.start()
    by_head = rows_first(lambda r: (r % 64) * 4 + r // 64)

    for step in range(8):
        both = mm(by_head, latent_ref[step]).astype(BF)
        for head in range(HEADS_DEV):
            split_ref[head, step * 64 : step * 64 + 64, :] = both[head * 64 : head * 64 + 64]
    loads[0].wait()
    for head in range(HEADS_DEV):
        lifted = mm(split_ref[head], up_ref[head]).astype(BF)
        lifted_ref[:, :, head * VHEAD : (head + 1) * VHEAD] = lifted.reshape(N_EP, 32, VHEAD)
    copies = []
    for band in range(4):
        for place in range(N_EP):
            picked_ref[place * 32 : place * 32 + 32, :] = lifted_ref[order_ref[band * N_EP + place]]
        loads[1 + band].wait()
        weight = weight_ref[:, band * BAND : (band + 1) * BAND]
        for half in (1, 0):
            part_ref[2 * band + half] = mm(
                picked_ref[half * 256 : half * 256 + 256, :], weight
            ).astype(BF)
            copies.append(
                pltpu.make_async_copy(
                    part_ref.at[2 * band + half], outs[2 * band + half], sems.at[2 * band + half]
                )
            )
            copies[-1].start()
    for copy in copies:
        copy.wait()


def project(order, latent, value_up, out_weight):
    whole = pl.BlockSpec(memory_space=pltpu.VMEM)
    far = pl.BlockSpec(memory_space=pltpu.HBM)
    return pl.pallas_call(
        project_body,
        in_specs=[pl.BlockSpec(memory_space=pltpu.SMEM), whole, far, far],
        out_specs=[pl.BlockSpec(memory_space=pltpu.HBM)] * 8,
        out_shape=[pltpu.HBM((256, BAND), BF)] * 8,
        scratch_shapes=[
            pltpu.VMEM((HEADS_DEV, 512, LAT), BF),
            pltpu.VMEM((N_EP, 32, 512), BF),
            pltpu.VMEM((512, 512), BF),
            pltpu.VMEM((8, 256, BAND), BF),
            pltpu.VMEM((HEADS_DEV, LAT, VHEAD), BF),
            pltpu.VMEM((512, D), BF),
            pltpu.SemaphoreType.DMA((5,)),
            pltpu.SemaphoreType.DMA((8,)),
        ],
        cost_estimate=pl.CostEstimate(
            flops=3 << 30, bytes_accessed=10 << 20, transcendentals=0
        ),
        compiler_params=pltpu.CompilerParams(vmem_limit_bytes=20 << 20),
        name="project",
    )(order, near(latent), distant(value_up), distant(out_weight))


def expert_body(x_ref, in_ref, out_ref, o_hbm, x_s, h_s, o_ref, sems):
    apart = rows_first(lambda r: (r % 128 // 4) * 8 + (r // 128) * 4 + r % 4)
    joined = rows_first(lambda r: (r // 4 % 2) * 128 + (r // 8) * 4 + r % 4)
    for step in range(4):
        block = mm(apart, x_ref[step * 256 : step * 256 + 256, :]).astype(BF)
        x_s[step * 128 : step * 128 + 128, :HALF] = block[:128]
        x_s[step * 128 : step * 128 + 128, HALF:] = block[128:]
    for at in range(0, FFE, 256):
        value = mm(x_s[...], in_ref[0, :, at : at + 256])
        h_s[:, at : at + 256] = (value / (1.0 + jnp.exp(-value))).astype(BF)
    copies = []
    for at in range(0, HALF, 256):
        halves = [
            mm(h_s[...], out_ref[0, :, first + at : first + at + 256]).astype(BF)
            for first in (0, HALF)
        ]
        for step in range(4):
            rows = slice(step * 128, step * 128 + 128)
            both = jnp.concatenate((halves[0][rows], halves[1][rows]), axis=0)
            o_ref[step * 256 : step * 256 + 256, at : at + 256] = mm(joined, both).astype(BF)
        copies.append(
            pltpu.make_async_copy(
                o_ref.at[:, pl.ds(at, 256)], o_hbm.at[:, pl.ds(at, 256)], sems.at[at // 256]
            )
        )
        copies[-1].start()
    for copy in copies:
        copy.wait()


def expert(incoming, expert_in, expert_out):
    whole = pl.BlockSpec(memory_space=pltpu.VMEM)
    return pl.pallas_call(
        expert_body,
        in_specs=[whole, whole, whole],
        out_specs=pl.BlockSpec(memory_space=pltpu.HBM),
        out_shape=pltpu.HBM((DEVICES * 8, HALF), BF),
        scratch_shapes=[
            pltpu.VMEM((512, D), BF),
            pltpu.VMEM((512, FFE), BF),
            pltpu.VMEM((DEVICES * 8, HALF), BF),
            pltpu.SemaphoreType.DMA((7,)),
        ],
        cost_estimate=pl.CostEstimate(
            flops=8 << 30, bytes_accessed=22 << 20, transcendentals=512 * 1024
        ),
        compiler_params=pltpu.CompilerParams(vmem_limit_bytes=24 << 20),
        name="expert",
    )(near(incoming), near(expert_in), near(expert_out))


NEAR = [(0, 1), (1, 0), (2, 3), (3, 2)]
FAR = [(0, 3), (3, 0), (1, 2), (2, 1)]
PAIRS = {1: NEAR, 3: FAR}
ROUTES = (
    (("ep_0", 1), ("ep_0", 3), ("ep_1", 1), ("ep_1", 3)),
    (("ep_0", 3), ("ep_0", 1), ("ep_1", 3), ("ep_1", 1)),
    (("ep_1", 1), ("ep_1", 3), ("ep_0", 1), ("ep_0", 3)),
    (("ep_1", 3), ("ep_1", 1), ("ep_0", 3), ("ep_0", 1)),
)


def block_order():
    first, second = [], []
    for route in ROUTES:
        places = [(0, 0)]
        for axis, flip in reversed(route):
            turn = (flip, 0) if axis == "ep_0" else (0, flip)
            places = places + [(a ^ turn[0], b ^ turn[1]) for a, b in places]
        first += [a for a, _ in places]
        second += [b for _, b in places]
    mine = lax.axis_index("ep_0"), lax.axis_index("ep_1")
    return (jnp.array(first, jnp.int32) ^ mine[0]) * 4 + (jnp.array(second, jnp.int32) ^ mine[1])


def sum_over_columns(parts):
    kept = [parts[2 * band] for band in range(4)]
    sent = [parts[2 * band + 1] for band in range(4)]
    arrived = [[] for _ in range(4)]
    rows = 256
    for step in range(4):
        for band in range(4):
            axis, flip = ROUTES[band][step]
            arrived[band].append(lax.ppermute(sent[band], axis, PAIRS[flip]))
        if step == 3:
            break
        rows //= 2
        for band in range(4):
            total = kept[band][rows : 2 * rows].astype(F32)
            for piece in arrived[band]:
                total = total + piece[rows : 2 * rows].astype(F32)
            sent[band] = total.astype(BF)
    sums = []
    for band in range(4):
        total = kept[band][:rows].astype(F32)
        for piece in arrived[band]:
            total = total + piece[:rows].astype(F32)
        sums.append(total)
    return jnp.concatenate(sums, axis=1)


def shifted(value, axis, steps):
    count = lax.axis_size(axis)
    return lax.ppermute(value, axis, [(s, (s + steps) % count) for s in range(count)])


def from_replicas(value):
    return jnp.concatenate([shifted(value, "rep", back) for back in range(1, 8)], axis=0)


def per_device(
    latent_pages,
    queries,
    residual,
    page_count,
    last_fill,
    page_order,
    shed_slots,
    shed_shift,
    expert_ids,
    gate_weight,
    expert_home,
    norm_gain,
    value_up,
    out_weight,
    expert_in,
    expert_out,
):
    replica = lax.axis_index("rep")
    own_counts = page_count[replica, 0, :]
    own_lengths = (own_counts - 1) * PAGE + last_fill[replica, 0, :]
    offsets = jnp.cumsum(own_counts) - own_counts
    latent = attention(page_order[0], offsets, own_lengths, queries, latent_pages)
    tokens = jnp.arange(TOK_DEV, dtype=jnp.int32)
    own_sheds = shed_slots[replica, 0, :]
    shed_rows = (own_sheds[:, None] * SPEC + jnp.arange(SPEC, dtype=jnp.int32)).reshape(-1)
    pick = shed_rows[:, None] == tokens[None, :]
    present = jnp.any(pick, axis=0)[:, None]
    wanted = jnp.arange(1, 8, dtype=jnp.int32)[:, None] == jnp.repeat(shed_shift[0], SPEC)[None, :]
    place = (wanted[:, :, None] & pick[None, :, :]).reshape(7 * 2 * SPEC, TOK_DEV).astype(BF)
    pick = pick.astype(BF)

    def offered(own):
        return from_replicas(mm(pick, own).astype(BF))

    def served(own, came):
        taken = lax.dot_general(place, came, (((0,), (0,)), ((), ())), preferred_element_type=F32)
        return jnp.where(present, taken.astype(BF), own)

    own_residual = residual.reshape(TOK_DEV, D)
    served_residual = served(own_residual, offered(own_residual))
    latent, served_residual = lax.optimization_barrier((latent, served_residual))
    gathered = lax.all_to_all(latent, EP, split_axis=0, concat_axis=0, tiled=True)
    parts = project(block_order(), gathered.reshape(8, 256, LAT), value_up, out_weight)
    own_branch = sum_over_columns(parts).astype(BF)

    served_branch = served(own_branch, offered(own_branch))
    mixed = served_residual.astype(F32) + served_branch.astype(F32)
    square = jnp.mean(mixed * mixed, axis=1, keepdims=True)
    normed = (mixed * lax.rsqrt(square + NORM_EPS) * norm_gain).astype(BF)

    target = expert_home[expert_ids.reshape(-1)]
    hits = (target[:, None] == jnp.arange(DEVICES, dtype=jnp.int32)[None, :]).astype(jnp.int32)
    before = jnp.sum((jnp.cumsum(hits, axis=0) - hits) * hits, axis=1)
    slot = (target * CAP + before).reshape(TOK_DEV, TOP)
    row = jnp.arange(DEVICES * 8, dtype=jnp.int32)
    row_slot = row // 8 * CAP + row % CAP
    row_half = row // CAP % 2
    both = jnp.arange(2 * TOK_DEV, dtype=jnp.int32)
    same_half = row_half[None, :] == (both // TOK_DEV)[:, None]
    landing = slot[:, :, None] == row_slot[None, None, :]
    chosen = jnp.any(landing, axis=1)
    chooser = (jnp.concatenate((chosen, chosen)) & same_half).astype(BF)
    gates = jnp.sum(jnp.where(landing, gate_weight[:, :, None], 0.0), axis=1)
    gates = jnp.where(same_half, jnp.concatenate((gates, gates)), 0.0)
    coarse = lax.reduce_precision(gates, 8, 7)
    gates = jnp.concatenate((coarse.astype(BF), (gates - coarse).astype(BF)))

    def halves(value):
        return jnp.concatenate((value[:, :HALF], value[:, HALF:]), axis=0)

    outgoing = lax.dot_general(
        chooser, halves(normed), (((0,), (0,)), ((), ())), preferred_element_type=F32
    ).astype(BF)
    incoming = lax.all_to_all(outgoing, REP_EP, split_axis=0, concat_axis=0, tiled=True)
    outer = expert(incoming, expert_in, expert_out)
    returned = lax.all_to_all(outer, REP_EP, split_axis=0, concat_axis=0, tiled=True)
    moe = mm(gates, returned)
    layer = (halves(mixed) + moe[: 2 * TOK_DEV] + moe[2 * TOK_DEV :]).astype(BF)
    layer_out = jnp.concatenate((layer[:TOK_DEV], layer[TOK_DEV:]), axis=1)
    return (
        served_branch.reshape(REQ_DEV, SPEC * D),
        layer_out.reshape(REQ_DEV, SPEC * D),
    )


def solution(mesh):
    torus = Mesh(mesh.devices.reshape(mesh.shape["rep"], 4, 4), ("rep", "ep_0", "ep_1"))
    return jax.shard_map(
        per_device,
        mesh=torus,
        in_specs=(
            P(REP_EP, None),
            P(REP_EP, None),
            P(REP_EP, None),
            P(None, EP, None),
            P(None, EP, None),
            P(REP_EP, None),
            P(None, EP, None),
            P(EP, None),
            P(REP_EP, None),
            P(REP_EP, None),
            P(),
            P(),
            P(EP, None, None),
            P(EP, None),
            P(REP_EP, None, None),
            P(REP_EP, None, None),
        ),
        out_specs=(P(REP_EP, None), P(REP_EP, None)),
        check_vma=False,
    )
```

```python
import functools

import jax
import jax.numpy as jnp
from jax import lax
from jax.experimental import pallas as pl
from jax.experimental.pallas import tpu as pltpu
from jax.sharding import Mesh
from jax.sharding import PartitionSpec as P

D = 3584
HALF = D // 2
HEADS = 64
LAT = 512
KVW = 576
VHEAD = 128
FFE = 1024
TOP = 8
PAGE = 64
SPEC = 4
MAXP = 12
REQ_DEV = 8
PAGES_DEV = 48
TOK_DEV = REQ_DEV * SPEC
N_EP = 16
HEADS_DEV = HEADS // N_EP
DEVICES = 128
CAP = 4
BAND = D // 4
KEYS = MAXP * PAGE
EP = ("ep_0", "ep_1")
REP_EP = ("rep", "ep_0", "ep_1")
SCORE_SCALE = 192.0 ** (-0.5)
NORM_EPS = 0.25
BF = jnp.bfloat16
F32 = jnp.float32


def iota2(rows, cols, dim):
    return lax.broadcasted_iota(jnp.int32, (rows, cols), dim)


def rows_first(source_of, size=256):
    return (iota2(size, size, 1) == source_of(iota2(size, size, 0))).astype(BF)


def mm(a, b):
    return jnp.dot(a, b, preferred_element_type=F32)


def near(value):
    return pltpu.with_memory_space_constraint(value, pltpu.VMEM)


def distant(value):
    return pltpu.with_memory_space_constraint(value, pltpu.HBM)


WINDOW = 12
SPAN = 8 * KVW


def attention_body(pick_ref, count_ref, fill_ref, query_hbm, page_hbm, out_hbm, *scratch):
    key_s, order_s, piece_s, query_s, page_v, query_v, out_ref = scratch[:7]
    page_sem, query_sem, out_sem = scratch[7:]

    def page_load(group):
        columns = pl.ds(pl.multiple_of(group * SPAN, 128), SPAN)
        return pltpu.make_async_copy(page_hbm.at[:, columns], page_v.at[group], page_sem.at[group])

    def query_load(position, pair):
        at = position * HEADS * KVW + pair * SPAN
        return pltpu.make_async_copy(
            query_hbm.at[:, pl.ds(pl.multiple_of(at, 128), SPAN)],
            query_v.at[pair, position],
            query_sem.at[pair, position],
        )

    def result_copy(i):
        rows = pl.ds(pl.multiple_of(i * 16, 16), 16)
        return pltpu.make_async_copy(out_ref.at[:, rows], out_hbm.at[:, rows], out_sem.at[i])

    for group in range(8):
        page_load(group).start()
    for pair in range(8):
        for position in range(SPEC):
            query_load(position, pair).start()
    shift = iota2(8, 128, 0) * PAGES_DEV
    for place in range(PAGES_DEV):
        order_s[place * 8 : place * 8 + 8, :] = shift + pick_ref[0, place]
    to_place = (iota2(384, 384, 1) == order_s[:, :1]).astype(BF)

    def regroup_keys(group, carry):
        page_load(group).wait()
        tokens = [page_v[group, :, t * KVW : (t + 1) * KVW] for t in range(8)]
        key_s[group] = mm(to_place, jnp.concatenate(tokens, axis=0))
        return carry

    lax.fori_loop(0, 8, regroup_keys, 0)
    row, col = iota2(REQ_DEV * 32, 256, 0), iota2(REQ_DEV * 32, 256, 1)
    by_request = (col == row % 32 * 8 + row // 32).astype(BF)

    def regroup_queries(pair, carry):
        for position in range(SPEC):
            query_load(position, pair).wait()
        for column in range(2):
            for position in range(SPEC):
                for head in range(HEADS_DEV):
                    at = (column * HEADS_DEV + head) * KVW
                    place = (column * SPEC + position) * HEADS_DEV + head
                    piece_s[place * 8 : place * 8 + 8, :] = query_v[
                        pair, position, :, at : at + KVW
                    ].astype(F32)
        rows = mm(by_request, piece_s[...].astype(BF)).astype(BF)
        query_s[:, pl.ds(pl.multiple_of(pair * 32, 32), 32), :] = rows.reshape(REQ_DEV, 32, KVW)
        return carry

    lax.fori_loop(0, 8, regroup_queries, 0)

    replica = lax.axis_index("rep")
    rows = SPEC * HEADS
    late = iota2(rows, 1, 0) // HEADS_DEV % SPEC - SPEC + 1
    key = iota2(1, KEYS, 1)
    place = key % (WINDOW * 8) // 8
    token = place * PAGE + key // (WINDOW * 8) * 8 + key % 8

    def request(i, offset):
        count = count_ref[replica, 0, i]
        length = (count - 1) * PAGE + fill_ref[replica, 0, i]
        start = jnp.minimum(offset, PAGES_DEV - WINDOW)
        skip = offset - start
        keys = key_s[:, pl.ds(pl.multiple_of(start * 8, 8), WINDOW * 8), :]
        keys = keys.reshape(KEYS, KVW).astype(BF)
        scores = lax.dot_general(
            query_s[i], keys, (((1,), (1,)), ((), ())), preferred_element_type=F32
        )
        at = jnp.where(place < skip, KEYS, token - skip * PAGE)
        scores = jnp.where(at < late + length, scores * SCORE_SCALE, -1e30)
        exponent = jnp.exp(scores - jnp.max(scores, axis=1, keepdims=True))
        total = jnp.sum(exponent, axis=1, keepdims=True)
        latent = mm(exponent.astype(BF), keys[:, :LAT]) / total
        out_ref[:, pl.ds(pl.multiple_of(i * 16, 16), 16), :] = latent.astype(BF).reshape(
            N_EP, 16, LAT
        )
        result_copy(i).start()
        return offset + count

    lax.fori_loop(0, REQ_DEV, request, jnp.int32(0))
    for i in range(REQ_DEV):
        result_copy(i).wait()


def attention(page_order, page_count, last_fill, queries, pages):
    few = pl.BlockSpec(memory_space=pltpu.SMEM)
    far = pl.BlockSpec(memory_space=pltpu.HBM)
    return pl.pallas_call(
        attention_body,
        in_specs=[few, few, few, far, far],
        out_specs=far,
        out_shape=pltpu.HBM((N_EP, REQ_DEV * 16, LAT), BF),
        scratch_shapes=[
            pltpu.VMEM((8, PAGES_DEV * 8, KVW), F32),
            pltpu.VMEM((PAGES_DEV * 8, 128), jnp.int32),
            pltpu.VMEM((256, KVW), F32),
            pltpu.VMEM((REQ_DEV, SPEC * HEADS, KVW), BF),
            pltpu.VMEM((8, PAGES_DEV, SPAN), BF),
            pltpu.VMEM((8, SPEC, REQ_DEV, SPAN), BF),
            pltpu.VMEM((N_EP, REQ_DEV * 16, LAT), BF),
            pltpu.SemaphoreType.DMA((8,)),
            pltpu.SemaphoreType.DMA((8, SPEC)),
            pltpu.SemaphoreType.DMA((REQ_DEV,)),
        ],
        cost_estimate=pl.CostEstimate(
            flops=7 << 30, bytes_accessed=8 << 20, transcendentals=8 * 256 * 768
        ),
        compiler_params=pltpu.CompilerParams(vmem_limit_bytes=40 << 20),
        name="attention",
    )(*[distant(each) for each in (page_order, page_count, last_fill, queries, pages)])


def weight_loads(weight_hbm, weight_ref, sems):
    loads = []
    for band in range(4):
        columns = pl.ds(band * BAND, BAND)
        loads.append(
            pltpu.make_async_copy(
                weight_hbm.at[:, columns], weight_ref.at[:, columns], sems.at[band]
            )
        )
        loads[-1].start()
    return loads


def part_of(order_ref, lifted_ref, picked_ref, weight_ref, load, band, first):
    for place in range(8):
        source = order_ref[band * N_EP + first + place]
        picked_ref[place * 32 : place * 32 + 32, :] = lifted_ref[source]
    load.wait()
    return mm(picked_ref[...], weight_ref[:, band * BAND : (band + 1) * BAND]).astype(BF)


def sent_body(order_ref, latent_ref, up_hbm, weight_hbm, *rest):
    outs, lifted_ref = rest[:4], rest[4]
    split_ref, picked_ref, part_ref, up_ref, weight_ref, in_sems, sems = rest[5:]
    up_load = pltpu.make_async_copy(up_hbm, up_ref, in_sems.at[4])
    up_load.start()
    loads = weight_loads(weight_hbm, weight_ref, in_sems)
    by_head = rows_first(lambda r: (r % 64) * 4 + r // 64)
    for step in range(8):
        both = mm(by_head, latent_ref[step]).astype(BF)
        for head in range(HEADS_DEV):
            split_ref[head, step * 64 : step * 64 + 64, :] = both[head * 64 : head * 64 + 64]
    up_load.wait()
    for head in range(HEADS_DEV):
        lifted = mm(split_ref[head], up_ref[head]).astype(BF)
        columns = slice(head * VHEAD, (head + 1) * VHEAD)
        lifted_ref[:, :, columns] = lifted.reshape(N_EP, 32, VHEAD)
    copies = []
    for band in range(4):
        part_ref[band] = part_of(
            order_ref, lifted_ref, picked_ref, weight_ref, loads[band], band, 8
        )
        copies.append(pltpu.make_async_copy(part_ref.at[band], outs[band], sems.at[band]))
        copies[-1].start()
    for copy in copies:
        copy.wait()


def kept_body(order_ref, lifted_ref, weight_hbm, out_ref, picked_ref, weight_ref, in_sems):
    loads = weight_loads(weight_hbm, weight_ref, in_sems)
    for band in range(4):
        out_ref[band] = part_of(
            order_ref, lifted_ref, picked_ref, weight_ref, loads[band], band, 0
        )


def project(order, latent, value_up, out_weight):
    few = pl.BlockSpec(memory_space=pltpu.SMEM)
    whole = pl.BlockSpec(memory_space=pltpu.VMEM)
    far = pl.BlockSpec(memory_space=pltpu.HBM)
    *sent, lifted = pl.pallas_call(
        sent_body,
        in_specs=[few, whole, far, far],
        out_specs=[far] * 4 + [whole],
        out_shape=[pltpu.HBM((256, BAND), BF)] * 4 + [pltpu.VMEM((N_EP, 32, 512), BF)],
        scratch_shapes=[
            pltpu.VMEM((HEADS_DEV, 512, LAT), BF),
            pltpu.VMEM((256, 512), BF),
            pltpu.VMEM((4, 256, BAND), BF),
            pltpu.VMEM((HEADS_DEV, LAT, VHEAD), BF),
            pltpu.VMEM((512, D), BF),
            pltpu.SemaphoreType.DMA((5,)),
            pltpu.SemaphoreType.DMA((4,)),
        ],
        cost_estimate=pl.CostEstimate(
            flops=2 << 30, bytes_accessed=8 << 20, transcendentals=0
        ),
        compiler_params=pltpu.CompilerParams(vmem_limit_bytes=20 << 20),
        name="project_sent",
    )(order, near(latent), distant(value_up), distant(out_weight))
    kept = pl.pallas_call(
        kept_body,
        in_specs=[few, whole, far],
        out_specs=whole,
        out_shape=pltpu.VMEM((4, 256, BAND), BF),
        scratch_shapes=[
            pltpu.VMEM((256, 512), BF),
            pltpu.VMEM((512, D), BF),
            pltpu.SemaphoreType.DMA((4,)),
        ],
        cost_estimate=pl.CostEstimate(
            flops=1 << 30, bytes_accessed=6 << 20, transcendentals=0
        ),
        compiler_params=pltpu.CompilerParams(vmem_limit_bytes=12 << 20),
        name="project_kept",
    )(order, near(lifted), distant(out_weight))
    return *sent, kept


def add_body(rows, split_at, joined, kept_ref, *rest):
    came, send, stay = rest[:split_at], rest[split_at:-1], rest[-1]
    split = 4 // split_at
    for band in range(4):
        piece = came[band // split]
        columns = slice(band % split * BAND, (band % split + 1) * BAND)
        total = kept_ref[band].astype(F32) + piece[:, columns].astype(F32)
        stay[band] = total[:rows]
        if joined:
            send[band // 2][:, band % 2 * BAND : (band % 2 + 1) * BAND] = total[rows:].astype(BF)
        else:
            send[band][...] = total[rows:].astype(BF)


def add_pieces(kept, came, joined):
    rows = kept.shape[1] // 2
    shape, count = ((rows, 2 * BAND), 2) if joined else ((rows, BAND), 4)
    whole = pl.BlockSpec(memory_space=pltpu.VMEM)
    outs = pl.pallas_call(
        functools.partial(add_body, rows, len(came), joined),
        in_specs=[whole] * (1 + len(came)),
        out_specs=[whole] * (count + 1),
        out_shape=[jax.ShapeDtypeStruct(shape, BF)] * count
        + [jax.ShapeDtypeStruct((4, rows, BAND), F32)],
        cost_estimate=pl.CostEstimate(
            flops=8 * rows * D, bytes_accessed=8 * rows * D, transcendentals=0
        ),
        compiler_params=pltpu.CompilerParams(vmem_limit_bytes=4 << 20),
        name="add_pieces",
    )(near(kept), *[near(piece) for piece in came])
    return outs[:-1], outs[-1]


def finish_body(pick_ref, kept_ref, first_ref, second_ref, own_ref, offer_ref):
    for band in range(4):
        piece = (first_ref, second_ref)[band // 2]
        columns = slice(band % 2 * BAND, (band % 2 + 1) * BAND)
        total = (kept_ref[band] + piece[:, columns].astype(F32)).astype(BF)
        own_ref[:, band * BAND : (band + 1) * BAND] = total
        offer_ref[:, band * BAND : (band + 1) * BAND] = mm(pick_ref[...], total).astype(BF)


def finish(pick, kept, first, second):
    whole = pl.BlockSpec(memory_space=pltpu.VMEM)
    return pl.pallas_call(
        finish_body,
        in_specs=[whole] * 4,
        out_specs=[whole] * 2,
        out_shape=[
            jax.ShapeDtypeStruct((TOK_DEV, D), BF),
            jax.ShapeDtypeStruct((2 * SPEC, D), BF),
        ],
        compiler_params=pltpu.CompilerParams(vmem_limit_bytes=4 << 20),
        cost_estimate=pl.CostEstimate(flops=4 << 20, bytes_accessed=1 << 20, transcendentals=0),
        name="finish",
    )(near(pick), near(kept), near(first), near(second))


def expert_body(x_ref, in_ref, out_ref, o_hbm, x_s, h_s, o_ref, sems):
    apart = rows_first(lambda r: (r % 128 // 4) * 8 + (r // 128) * 4 + r % 4)
    joined = rows_first(lambda r: (r // 4 % 2) * 128 + (r // 8) * 4 + r % 4)
    for step in range(4):
        block = mm(apart, x_ref[step * 256 : step * 256 + 256, :]).astype(BF)
        x_s[step * 128 : step * 128 + 128, :HALF] = block[:128]
        x_s[step * 128 : step * 128 + 128, HALF:] = block[128:]
    for at in range(0, FFE, 256):
        value = mm(x_s[...], in_ref[0, :, at : at + 256])
        h_s[:, at : at + 256] = (value / (1.0 + jnp.exp(-value))).astype(BF)
    copies = []
    for at in range(0, HALF, 256):
        halves = [
            mm(h_s[...], out_ref[0, :, first + at : first + at + 256]).astype(BF)
            for first in (0, HALF)
        ]
        for step in range(4):
            rows = slice(step * 128, step * 128 + 128)
            both = jnp.concatenate((halves[0][rows], halves[1][rows]), axis=0)
            o_ref[step * 256 : step * 256 + 256, at : at + 256] = mm(joined, both).astype(BF)
        copies.append(
            pltpu.make_async_copy(
                o_ref.at[:, pl.ds(at, 256)], o_hbm.at[:, pl.ds(at, 256)], sems.at[at // 256]
            )
        )
        copies[-1].start()
    for copy in copies:
        copy.wait()


def expert(incoming, expert_in, expert_out):
    whole = pl.BlockSpec(memory_space=pltpu.VMEM)
    return pl.pallas_call(
        expert_body,
        in_specs=[whole, whole, whole],
        out_specs=pl.BlockSpec(memory_space=pltpu.HBM),
        out_shape=pltpu.HBM((DEVICES * 8, HALF), BF),
        scratch_shapes=[
            pltpu.VMEM((512, D), BF),
            pltpu.VMEM((512, FFE), BF),
            pltpu.VMEM((DEVICES * 8, HALF), BF),
            pltpu.SemaphoreType.DMA((7,)),
        ],
        cost_estimate=pl.CostEstimate(
            flops=8 << 30, bytes_accessed=22 << 20, transcendentals=512 * 1024
        ),
        compiler_params=pltpu.CompilerParams(vmem_limit_bytes=24 << 20),
        name="expert",
    )(near(incoming), near(expert_in), near(expert_out))


NEAR = [(0, 1), (1, 0), (2, 3), (3, 2)]
FAR = [(0, 3), (3, 0), (1, 2), (2, 1)]
PAIRS = {1: NEAR, 3: FAR}
ROUTES = (
    (("ep_0", 1), ("ep_0", 3), ("ep_1", 1), ("ep_1", 3)),
    (("ep_0", 3), ("ep_0", 1), ("ep_1", 1), ("ep_1", 3)),
    (("ep_1", 1), ("ep_1", 3), ("ep_0", 1), ("ep_0", 3)),
    (("ep_1", 3), ("ep_1", 1), ("ep_0", 1), ("ep_0", 3)),
)


def block_order():
    first, second = [], []
    for route in ROUTES:
        places = [(0, 0)]
        for axis, flip in reversed(route):
            turn = (flip, 0) if axis == "ep_0" else (0, flip)
            places = places + [(a ^ turn[0], b ^ turn[1]) for a, b in places]
        first += [a for a, _ in places]
        second += [b for _, b in places]
    mine = lax.axis_index("ep_0"), lax.axis_index("ep_1")
    return (jnp.array(first, jnp.int32) ^ mine[0]) * 4 + (jnp.array(second, jnp.int32) ^ mine[1])


def exchange(pieces, step):
    every = 4 // len(pieces)
    out = []
    for at, piece in enumerate(pieces):
        axis, flip = ROUTES[at * every][step]
        out.append(lax.ppermute(piece, axis, PAIRS[flip]))
    return out


def sum_over_columns(pick, parts):
    *send, kept = parts
    for step in range(3):
        send, kept = add_pieces(kept, exchange(send, step), joined=step > 0)
    return finish(pick, kept, *exchange(send, 3))


def shifted(value, axis, steps):
    count = lax.axis_size(axis)
    return lax.ppermute(value, axis, [(s, (s + steps) % count) for s in range(count)])


def from_replicas(value):
    return jnp.concatenate([shifted(value, "rep", back) for back in range(1, 8)], axis=0)


def per_device(
    latent_pages,
    queries,
    residual,
    page_count,
    last_fill,
    page_order,
    shed_slots,
    shed_shift,
    expert_ids,
    gate_weight,
    expert_home,
    norm_gain,
    value_up,
    out_weight,
    expert_in,
    expert_out,
):
    replica = lax.axis_index("rep")
    latent = attention(page_order, page_count, last_fill, queries, latent_pages)
    latent = lax.all_to_all(latent, EP, split_axis=0, concat_axis=0, tiled=True)
    tokens = jnp.arange(TOK_DEV, dtype=jnp.int32)
    own_sheds = shed_slots[replica, 0, :]
    shed_rows = (own_sheds[:, None] * SPEC + jnp.arange(SPEC, dtype=jnp.int32)).reshape(-1)
    pick = shed_rows[:, None] == tokens[None, :]
    present = jnp.any(pick, axis=0)[:, None]
    wanted = jnp.arange(1, 8, dtype=jnp.int32)[:, None] == jnp.repeat(shed_shift[0], SPEC)[None, :]
    place = (wanted[:, :, None] & pick[None, :, :]).reshape(7 * 2 * SPEC, TOK_DEV).astype(BF)
    pick = pick.astype(BF)

    def served(own, came):
        taken = lax.dot_general(place, came, (((0,), (0,)), ((), ())), preferred_element_type=F32)
        return jnp.where(present, taken.astype(BF), own)

    own_residual = residual.reshape(TOK_DEV, D)
    came = from_replicas(mm(pick, own_residual).astype(BF))
    served_residual = served(own_residual, came)
    own_branch, offer = sum_over_columns(
        pick, project(block_order(), latent.reshape(8, 256, LAT), value_up, out_weight)
    )
    served_branch = served(own_branch, from_replicas(offer))
    mixed = served_residual.astype(F32) + served_branch.astype(F32)
    square = jnp.mean(mixed * mixed, axis=1, keepdims=True)
    normed = (mixed * lax.rsqrt(square + NORM_EPS) * norm_gain).astype(BF)

    target = expert_home[expert_ids.reshape(-1)]
    hits = (target[:, None] == jnp.arange(DEVICES, dtype=jnp.int32)[None, :]).astype(jnp.int32)
    before = jnp.sum((jnp.cumsum(hits, axis=0) - hits) * hits, axis=1)
    slot = (target * CAP + before).reshape(TOK_DEV, TOP)
    row = jnp.arange(DEVICES * 8, dtype=jnp.int32)
    row_slot = row // 8 * CAP + row % CAP
    row_half = row // CAP % 2
    both = jnp.arange(2 * TOK_DEV, dtype=jnp.int32)
    same_half = row_half[None, :] == (both // TOK_DEV)[:, None]
    landing = slot[:, :, None] == row_slot[None, None, :]
    chosen = jnp.any(landing, axis=1)
    chooser = (jnp.concatenate((chosen, chosen)) & same_half).astype(BF)
    gates = jnp.sum(jnp.where(landing, gate_weight[:, :, None], 0.0), axis=1)
    gates = jnp.where(same_half, jnp.concatenate((gates, gates)), 0.0)
    coarse = lax.reduce_precision(gates, 8, 7)
    gates = jnp.concatenate((coarse.astype(BF), (gates - coarse).astype(BF)))

    def halves(value):
        return jnp.concatenate((value[:, :HALF], value[:, HALF:]), axis=0)

    outgoing = lax.dot_general(
        chooser, halves(normed), (((0,), (0,)), ((), ())), preferred_element_type=F32
    ).astype(BF)
    incoming = lax.all_to_all(outgoing, REP_EP, split_axis=0, concat_axis=0, tiled=True)
    outer = expert(incoming, expert_in, expert_out)
    returned = lax.all_to_all(outer, REP_EP, split_axis=0, concat_axis=0, tiled=True)
    moe = mm(gates, returned)
    layer = (halves(mixed) + moe[: 2 * TOK_DEV] + moe[2 * TOK_DEV :]).astype(BF)
    layer_out = jnp.concatenate((layer[:TOK_DEV], layer[TOK_DEV:]), axis=1)
    return (
        served_branch.reshape(REQ_DEV, SPEC * D),
        layer_out.reshape(REQ_DEV, SPEC * D),
    )


def solution(mesh):
    torus = Mesh(mesh.devices.reshape(mesh.shape["rep"], 4, 4), ("rep", "ep_0", "ep_1"))

    return jax.shard_map(
        per_device,
        mesh=torus,
        in_specs=(
            P(REP_EP, None),
            P(REP_EP, None),
            P(REP_EP, None),
            P(None, EP, None),
            P(None, EP, None),
            P(REP_EP, None),
            P(None, EP, None),
            P(EP, None),
            P(REP_EP, None),
            P(REP_EP, None),
            P(),
            P(),
            P(EP, None, None),
            P(EP, None),
            P(REP_EP, None, None),
            P(REP_EP, None, None),
        ),
        out_specs=(P(REP_EP, None), P(REP_EP, None)),
        check_vma=False,
    )
```

```python
import functools

import jax
import jax.numpy as jnp
from jax import lax
from jax.experimental import pallas as pl
from jax.experimental.pallas import tpu as pltpu
from jax.sharding import Mesh
from jax.sharding import PartitionSpec as P

D = 3584
HALF = D // 2
HEADS = 64
LAT = 512
KVW = 576
VHEAD = 128
FFE = 1024
TOP = 8
PAGE = 64
SPEC = 4
MAXP = 12
REQ_DEV = 8
PAGES_DEV = 48
TOK_DEV = REQ_DEV * SPEC
N_EP = 16
HEADS_DEV = HEADS // N_EP
DEVICES = 128
CAP = 4
BAND = D // 4
KEYS = MAXP * PAGE
EP = ("ep_0", "ep_1")
REP_EP = ("rep", "ep_0", "ep_1")
SCORE_SCALE = 192.0 ** (-0.5)
NORM_EPS = 0.25
BF = jnp.bfloat16
F32 = jnp.float32


def iota2(rows, cols, dim):
    return lax.broadcasted_iota(jnp.int32, (rows, cols), dim)


def rows_first(source_of, size=256):
    return (iota2(size, size, 1) == source_of(iota2(size, size, 0))).astype(BF)


def mm(a, b):
    return jnp.dot(a, b, preferred_element_type=F32)


def near(value):
    return pltpu.with_memory_space_constraint(value, pltpu.VMEM)


def distant(value):
    return pltpu.with_memory_space_constraint(value, pltpu.HBM)


WINDOWS = (4, 8, 12, 14)
SPAN = 8 * KVW


def attention_body(pick_ref, count_ref, fill_ref, query_hbm, page_hbm, out_hbm, *scratch):
    key_s, order_s, piece_s, query_s, page_v, query_v, out_ref = scratch[:7]
    page_sem, query_sem, out_sem = scratch[7:]

    def page_load(group):
        columns = pl.ds(pl.multiple_of(group * SPAN, 128), SPAN)
        return pltpu.make_async_copy(page_hbm.at[:, columns], page_v.at[group], page_sem.at[group])

    def query_load(position, pair):
        at = position * HEADS * KVW + pair * SPAN
        return pltpu.make_async_copy(
            query_hbm.at[:, pl.ds(pl.multiple_of(at, 128), SPAN)],
            query_v.at[pair, position],
            query_sem.at[pair, position],
        )

    def result_copy(i):
        rows = pl.ds(pl.multiple_of(i * 16, 16), 16)
        return pltpu.make_async_copy(out_ref.at[:, rows], out_hbm.at[:, rows], out_sem.at[i])

    for group in range(8):
        page_load(group).start()
    for pair in range(8):
        for position in range(SPEC):
            query_load(position, pair).start()
    row = iota2(8, 128, 0)
    for place in range(0, PAGES_DEV, 2):
        page = jnp.where(row < 4, pick_ref[0, place], pick_ref[0, place + 1])
        order_s[place * 4 : place * 4 + 8, :] = row % 4 * PAGES_DEV + page
    to_place = (iota2(192, 192, 1) == order_s[:, :1]).astype(BF)

    def regroup_keys(group, carry):
        page_load(group).wait()
        for part in range(2):
            tokens = [
                page_v[group, :, t * KVW : (t + 1) * KVW] for t in range(4 * part, 4 * part + 4)
            ]
            key_s[group * 2 + part] = mm(to_place, jnp.concatenate(tokens, axis=0))
        return carry

    lax.fori_loop(0, 8, regroup_keys, 0)
    row, col = iota2(REQ_DEV * 32, 256, 0), iota2(REQ_DEV * 32, 256, 1)
    by_request = (col == row % 32 * 8 + row // 32).astype(BF)

    def regroup_queries(pair, carry):
        for position in range(SPEC):
            query_load(position, pair).wait()
        for column in range(2):
            for position in range(SPEC):
                for head in range(HEADS_DEV):
                    at = (column * HEADS_DEV + head) * KVW
                    place = (column * SPEC + position) * HEADS_DEV + head
                    piece_s[place * 8 : place * 8 + 8, :] = query_v[
                        pair, position, :, at : at + KVW
                    ].astype(F32)
        rows = mm(by_request, piece_s[...].astype(BF)).astype(BF)
        query_s[:, pl.ds(pl.multiple_of(pair * 32, 32), 32), :] = rows.reshape(REQ_DEV, 32, KVW)
        return carry

    lax.fori_loop(0, 8, regroup_queries, 0)

    replica = lax.axis_index("rep")
    rows = SPEC * HEADS
    late = iota2(rows, 1, 0) // HEADS_DEV % SPEC - SPEC + 1

    def attend(i, offset, length, window):
        start = jnp.minimum(offset // 2 * 2, PAGES_DEV - window)
        skip = offset - start
        span = window * 4
        keys = key_s[:, pl.ds(pl.multiple_of(start * 4, 8), span), :]
        keys = keys.reshape(16 * span, KVW).astype(BF)
        scores = lax.dot_general(
            query_s[i], keys, (((1,), (1,)), ((), ())), preferred_element_type=F32
        )
        key = iota2(1, 16 * span, 1)
        place = key % span // 4
        token = (place - skip) * PAGE + key // span * 4 + key % 4
        at = jnp.where(place < skip, KEYS, token)
        scores = jnp.where(at < late + length, scores * SCORE_SCALE, -1e30)
        exponent = jnp.exp(scores - jnp.max(scores, axis=1, keepdims=True))
        total = jnp.sum(exponent, axis=1, keepdims=True)
        latent = mm(exponent.astype(BF), keys[:, :LAT]) / total
        out_ref[:, pl.ds(pl.multiple_of(i * 16, 16), 16), :] = latent.astype(BF).reshape(
            N_EP, 16, LAT
        )

    def request(i, offset):
        count = count_ref[replica, 0, i]
        length = (count - 1) * PAGE + fill_ref[replica, 0, i]
        need = count + offset % 2
        for least, window in zip((0,) + WINDOWS, WINDOWS):
            pl.when((need > least) & (need <= window))(
                functools.partial(attend, i, offset, length, window)
            )
        result_copy(i).start()
        return offset + count

    lax.fori_loop(0, REQ_DEV, request, jnp.int32(0))
    for i in range(REQ_DEV):
        result_copy(i).wait()


def attention(page_order, page_count, last_fill, queries, pages):
    few = pl.BlockSpec(memory_space=pltpu.SMEM)
    far = pl.BlockSpec(memory_space=pltpu.HBM)
    return pl.pallas_call(
        attention_body,
        in_specs=[few, few, few, far, far],
        out_specs=far,
        out_shape=pltpu.HBM((N_EP, REQ_DEV * 16, LAT), BF),
        scratch_shapes=[
            pltpu.VMEM((16, PAGES_DEV * 4, KVW), F32),
            pltpu.VMEM((PAGES_DEV * 4, 128), jnp.int32),
            pltpu.VMEM((256, KVW), F32),
            pltpu.VMEM((REQ_DEV, SPEC * HEADS, KVW), BF),
            pltpu.VMEM((8, PAGES_DEV, SPAN), BF),
            pltpu.VMEM((8, SPEC, REQ_DEV, SPAN), BF),
            pltpu.VMEM((N_EP, REQ_DEV * 16, LAT), BF),
            pltpu.SemaphoreType.DMA((8,)),
            pltpu.SemaphoreType.DMA((8, SPEC)),
            pltpu.SemaphoreType.DMA((REQ_DEV,)),
        ],
        cost_estimate=pl.CostEstimate(
            flops=7 << 30, bytes_accessed=8 << 20, transcendentals=8 * 256 * 768
        ),
        compiler_params=pltpu.CompilerParams(vmem_limit_bytes=40 << 20),
        name="attention",
    )(*[distant(each) for each in (page_order, page_count, last_fill, queries, pages)])


def weight_loads(weight_hbm, weight_ref, sems):
    loads = []
    for band in range(4):
        columns = pl.ds(band * BAND, BAND)
        loads.append(
            pltpu.make_async_copy(
                weight_hbm.at[:, columns], weight_ref.at[:, columns], sems.at[band]
            )
        )
        loads[-1].start()
    return loads


def part_of(order_ref, lifted_ref, picked_ref, weight_ref, load, band, first):
    for place in range(8):
        source = order_ref[band * N_EP + first + place]
        picked_ref[place * 32 : place * 32 + 32, :] = lifted_ref[source]
    load.wait()
    return mm(picked_ref[...], weight_ref[:, band * BAND : (band + 1) * BAND]).astype(BF)


def sent_body(order_ref, latent_ref, up_hbm, weight_hbm, *rest):
    outs, lifted_ref = rest[:4], rest[4]
    split_ref, picked_ref, part_ref, up_ref, weight_ref, in_sems, sems = rest[5:]
    up_load = pltpu.make_async_copy(up_hbm, up_ref, in_sems.at[4])
    up_load.start()
    loads = weight_loads(weight_hbm, weight_ref, in_sems)
    by_head = rows_first(
        lambda r: (r // 32 % 2) * 128 + (r % 8) * 16 + (r // 8 % 4) * 4 + r // 64
    )
    for step in range(8):
        both = mm(by_head, latent_ref[step]).astype(BF)
        for head in range(HEADS_DEV):
            split_ref[head, step * 64 : step * 64 + 64, :] = both[head * 64 : head * 64 + 64]
    up_load.wait()
    for head in range(HEADS_DEV):
        lifted = mm(split_ref[head], up_ref[head]).astype(BF)
        columns = slice(head * VHEAD, (head + 1) * VHEAD)
        lifted_ref[:, :, columns] = lifted.reshape(N_EP, 32, VHEAD)
    copies = []
    for band in range(4):
        part_ref[band] = part_of(
            order_ref, lifted_ref, picked_ref, weight_ref, loads[band], band, 8
        )
        copies.append(pltpu.make_async_copy(part_ref.at[band], outs[band], sems.at[band]))
        copies[-1].start()
    for copy in copies:
        copy.wait()


def kept_body(order_ref, lifted_ref, weight_hbm, out_ref, picked_ref, weight_ref, in_sems):
    loads = weight_loads(weight_hbm, weight_ref, in_sems)
    for band in range(4):
        out_ref[band] = part_of(
            order_ref, lifted_ref, picked_ref, weight_ref, loads[band], band, 0
        )


def project(order, latent, value_up, out_weight):
    few = pl.BlockSpec(memory_space=pltpu.SMEM)
    whole = pl.BlockSpec(memory_space=pltpu.VMEM)
    far = pl.BlockSpec(memory_space=pltpu.HBM)
    *sent, lifted = pl.pallas_call(
        sent_body,
        in_specs=[few, whole, far, far],
        out_specs=[far] * 4 + [whole],
        out_shape=[pltpu.HBM((256, BAND), BF)] * 4 + [pltpu.VMEM((N_EP, 32, 512), BF)],
        scratch_shapes=[
            pltpu.VMEM((HEADS_DEV, 512, LAT), BF),
            pltpu.VMEM((256, 512), BF),
            pltpu.VMEM((4, 256, BAND), BF),
            pltpu.VMEM((HEADS_DEV, LAT, VHEAD), BF),
            pltpu.VMEM((512, D), BF),
            pltpu.SemaphoreType.DMA((5,)),
            pltpu.SemaphoreType.DMA((4,)),
        ],
        cost_estimate=pl.CostEstimate(
            flops=2 << 30, bytes_accessed=8 << 20, transcendentals=0
        ),
        compiler_params=pltpu.CompilerParams(vmem_limit_bytes=20 << 20),
        name="project_sent",
    )(order, near(latent), distant(value_up), distant(out_weight))
    kept = pl.pallas_call(
        kept_body,
        in_specs=[few, whole, far],
        out_specs=whole,
        out_shape=pltpu.VMEM((4, 256, BAND), BF),
        scratch_shapes=[
            pltpu.VMEM((256, 512), BF),
            pltpu.VMEM((512, D), BF),
            pltpu.SemaphoreType.DMA((4,)),
        ],
        cost_estimate=pl.CostEstimate(
            flops=1 << 30, bytes_accessed=6 << 20, transcendentals=0
        ),
        compiler_params=pltpu.CompilerParams(vmem_limit_bytes=12 << 20),
        name="project_kept",
    )(order, near(lifted), distant(out_weight))
    return *sent, kept


def add_body(rows, split_at, joined, kept_ref, *rest):
    came, send, stay = rest[:split_at], rest[split_at:-1], rest[-1]
    split = 4 // split_at
    for band in range(4):
        piece = came[band // split]
        columns = slice(band % split * BAND, (band % split + 1) * BAND)
        total = kept_ref[band].astype(F32) + piece[:, columns].astype(F32)
        stay[band] = total[:rows]
        if joined:
            send[band // 2][:, band % 2 * BAND : (band % 2 + 1) * BAND] = total[rows:].astype(BF)
        else:
            send[band][...] = total[rows:].astype(BF)


def add_pieces(kept, came, joined):
    rows = kept.shape[1] // 2
    shape, count = ((rows, 2 * BAND), 2) if joined else ((rows, BAND), 4)
    whole = pl.BlockSpec(memory_space=pltpu.VMEM)
    outs = pl.pallas_call(
        functools.partial(add_body, rows, len(came), joined),
        in_specs=[whole] * (1 + len(came)),
        out_specs=[whole] * (count + 1),
        out_shape=[jax.ShapeDtypeStruct(shape, BF)] * count
        + [jax.ShapeDtypeStruct((4, rows, BAND), F32)],
        cost_estimate=pl.CostEstimate(
            flops=8 * rows * D, bytes_accessed=8 * rows * D, transcendentals=0
        ),
        compiler_params=pltpu.CompilerParams(vmem_limit_bytes=4 << 20),
        name="add_pieces",
    )(near(kept), *[near(piece) for piece in came])
    return outs[:-1], outs[-1]


def finish_body(pick_ref, kept_ref, first_ref, second_ref, own_ref, offer_ref):
    for band in range(4):
        piece = (first_ref, second_ref)[band // 2]
        columns = slice(band % 2 * BAND, (band % 2 + 1) * BAND)
        total = (kept_ref[band] + piece[:, columns].astype(F32)).astype(BF)
        own_ref[:, band * BAND : (band + 1) * BAND] = total
        offer_ref[:, band * BAND : (band + 1) * BAND] = mm(pick_ref[...], total).astype(BF)


def finish(pick, kept, first, second):
    whole = pl.BlockSpec(memory_space=pltpu.VMEM)
    return pl.pallas_call(
        finish_body,
        in_specs=[whole] * 4,
        out_specs=[whole] * 2,
        out_shape=[
            jax.ShapeDtypeStruct((TOK_DEV, D), BF),
            jax.ShapeDtypeStruct((2 * SPEC, D), BF),
        ],
        compiler_params=pltpu.CompilerParams(vmem_limit_bytes=4 << 20),
        cost_estimate=pl.CostEstimate(flops=4 << 20, bytes_accessed=1 << 20, transcendentals=0),
        name="finish",
    )(near(pick), near(kept), near(first), near(second))


def expert_body(x_ref, in_ref, out_ref, o_hbm, x_s, h_s, o_ref, sems):
    apart = rows_first(lambda r: (r % 128 // 4) * 8 + (r // 128) * 4 + r % 4)
    joined = rows_first(lambda r: (r // 4 % 2) * 128 + (r // 8) * 4 + r % 4)
    for step in range(4):
        block = mm(apart, x_ref[step * 256 : step * 256 + 256, :]).astype(BF)
        x_s[step * 128 : step * 128 + 128, :HALF] = block[:128]
        x_s[step * 128 : step * 128 + 128, HALF:] = block[128:]
    for at in range(0, FFE, 256):
        value = mm(x_s[...], in_ref[0, :, at : at + 256])
        h_s[:, at : at + 256] = (value / (1.0 + jnp.exp(-value))).astype(BF)
    copies = []
    for at in range(0, HALF, 256):
        halves = [
            mm(h_s[...], out_ref[0, :, first + at : first + at + 256]).astype(BF)
            for first in (0, HALF)
        ]
        for step in range(4):
            rows = slice(step * 128, step * 128 + 128)
            both = jnp.concatenate((halves[0][rows], halves[1][rows]), axis=0)
            o_ref[step * 256 : step * 256 + 256, at : at + 256] = mm(joined, both).astype(BF)
        copies.append(
            pltpu.make_async_copy(
                o_ref.at[:, pl.ds(at, 256)], o_hbm.at[:, pl.ds(at, 256)], sems.at[at // 256]
            )
        )
        copies[-1].start()
    for copy in copies:
        copy.wait()


def expert(incoming, expert_in, expert_out):
    whole = pl.BlockSpec(memory_space=pltpu.VMEM)
    return pl.pallas_call(
        expert_body,
        in_specs=[whole, whole, whole],
        out_specs=pl.BlockSpec(memory_space=pltpu.HBM),
        out_shape=pltpu.HBM((DEVICES * 8, HALF), BF),
        scratch_shapes=[
            pltpu.VMEM((512, D), BF),
            pltpu.VMEM((512, FFE), BF),
            pltpu.VMEM((DEVICES * 8, HALF), BF),
            pltpu.SemaphoreType.DMA((7,)),
        ],
        cost_estimate=pl.CostEstimate(
            flops=8 << 30, bytes_accessed=22 << 20, transcendentals=512 * 1024
        ),
        compiler_params=pltpu.CompilerParams(vmem_limit_bytes=24 << 20),
        name="expert",
    )(near(incoming), near(expert_in), near(expert_out))


NEAR = [(0, 1), (1, 0), (2, 3), (3, 2)]
FAR = [(0, 3), (3, 0), (1, 2), (2, 1)]
PAIRS = {1: NEAR, 3: FAR}
ROUTES = (
    (("ep_0", 1), ("ep_0", 3), ("ep_1", 1), ("ep_1", 3)),
    (("ep_0", 3), ("ep_0", 1), ("ep_1", 1), ("ep_1", 3)),
    (("ep_1", 1), ("ep_1", 3), ("ep_0", 1), ("ep_0", 3)),
    (("ep_1", 3), ("ep_1", 1), ("ep_0", 1), ("ep_0", 3)),
)


def block_order():
    first, second = [], []
    for route in ROUTES:
        places = [(0, 0)]
        for axis, flip in reversed(route):
            turn = (flip, 0) if axis == "ep_0" else (0, flip)
            places = places + [(a ^ turn[0], b ^ turn[1]) for a, b in places]
        first += [a for a, _ in places]
        second += [b for _, b in places]
    mine = lax.axis_index("ep_0"), lax.axis_index("ep_1")
    return (jnp.array(first, jnp.int32) ^ mine[0]) * 4 + (jnp.array(second, jnp.int32) ^ mine[1])


def exchange(pieces, step):
    every = 4 // len(pieces)
    out = []
    for at, piece in enumerate(pieces):
        axis, flip = ROUTES[at * every][step]
        out.append(lax.ppermute(piece, axis, PAIRS[flip]))
    return out


def sum_over_columns(pick, parts):
    *send, kept = parts
    for step in range(3):
        send, kept = add_pieces(kept, exchange(send, step), joined=step > 0)
    return finish(pick, kept, *exchange(send, 3))


def shifted(value, axis, steps):
    count = lax.axis_size(axis)
    return lax.ppermute(value, axis, [(s, (s + steps) % count) for s in range(count)])


def from_replicas(value, odd):
    crossed = lax.ppermute(value, "rep", [(i, i ^ 1) for i in range(8)])
    value = jnp.where(odd, crossed, value)
    planes = [shifted(value, "rep", 2 * back) for back in range(1, 4)]
    return jnp.concatenate([value] + planes, axis=0)


def by_position(value):
    return jnp.concatenate([value[:, s * D : (s + 1) * D] for s in range(SPEC)], axis=0)


def by_slot(value):
    return jnp.concatenate([value[s * REQ_DEV : (s + 1) * REQ_DEV] for s in range(SPEC)], axis=1)


def per_device(
    latent_pages,
    queries,
    residual,
    page_count,
    last_fill,
    page_order,
    shed_slots,
    shed_shift,
    expert_ids,
    gate_weight,
    expert_home,
    norm_gain,
    value_up,
    out_weight,
    expert_in,
    expert_out,
):
    replica = lax.axis_index("rep")
    latent = attention(page_order, page_count, last_fill, queries, latent_pages)
    latent = lax.all_to_all(latent, EP, split_axis=0, concat_axis=0, tiled=True)
    tokens = jnp.arange(TOK_DEV, dtype=jnp.int32)
    own_sheds = shed_slots[replica, 0, :]
    shed_rows = (jnp.arange(SPEC, dtype=jnp.int32) * REQ_DEV + own_sheds[:, None]).reshape(-1)
    pick = shed_rows[:, None] == tokens[None, :]
    present = jnp.any(pick, axis=0)[:, None]
    row_shifts = jnp.repeat(shed_shift[0], SPEC)
    odd = (row_shifts % 2 == 1)[:, None]
    planes = (row_shifts + 1 - replica % 2) // 2 % 4
    wanted = jnp.arange(4, dtype=jnp.int32)[:, None] == planes[None, :]
    place = (wanted[:, :, None] & pick[None, :, :]).reshape(4 * 2 * SPEC, TOK_DEV).astype(BF)
    pick = pick.astype(BF)

    def served(own, came):
        taken = lax.dot_general(place, came, (((0,), (0,)), ((), ())), preferred_element_type=F32)
        return jnp.where(present, taken.astype(BF), own)

    own_residual = by_position(residual)
    came = from_replicas(mm(pick, own_residual).astype(BF), odd)
    served_residual = served(own_residual, came)
    own_branch, offer = sum_over_columns(
        pick, project(block_order(), latent.reshape(8, 256, LAT), value_up, out_weight)
    )
    served_branch = served(own_branch, from_replicas(offer, odd))
    mixed = served_residual.astype(F32) + served_branch.astype(F32)
    square = jnp.mean(mixed * mixed, axis=1, keepdims=True)
    normed = (mixed * lax.rsqrt(square + NORM_EPS) * norm_gain).astype(BF)

    def routed(value):
        return value.reshape(REQ_DEV, SPEC, TOP).transpose(1, 0, 2).reshape(TOK_DEV, TOP)

    gate_weight = routed(gate_weight)
    target = expert_home[routed(expert_ids).reshape(-1)]
    hits = (target[:, None] == jnp.arange(DEVICES, dtype=jnp.int32)[None, :]).astype(jnp.int32)
    before = jnp.sum((jnp.cumsum(hits, axis=0) - hits) * hits, axis=1)
    slot = (target * CAP + before).reshape(TOK_DEV, TOP)
    row = jnp.arange(DEVICES * 8, dtype=jnp.int32)
    row_slot = row // 8 * CAP + row % CAP
    row_half = row // CAP % 2
    both = jnp.arange(2 * TOK_DEV, dtype=jnp.int32)
    same_half = row_half[None, :] == (both // TOK_DEV)[:, None]
    landing = slot[:, :, None] == row_slot[None, None, :]
    chosen = jnp.any(landing, axis=1)
    chooser = (jnp.concatenate((chosen, chosen)) & same_half).astype(BF)
    gates = jnp.sum(jnp.where(landing, gate_weight[:, :, None], 0.0), axis=1)
    gates = jnp.where(same_half, jnp.concatenate((gates, gates)), 0.0)
    coarse = lax.reduce_precision(gates, 8, 7)
    gates = jnp.concatenate((coarse.astype(BF), (gates - coarse).astype(BF)))

    def halves(value):
        return jnp.concatenate((value[:, :HALF], value[:, HALF:]), axis=0)

    outgoing = lax.dot_general(
        chooser, halves(normed), (((0,), (0,)), ((), ())), preferred_element_type=F32
    ).astype(BF)
    incoming = lax.all_to_all(outgoing, REP_EP, split_axis=0, concat_axis=0, tiled=True)
    outer = expert(incoming, expert_in, expert_out)
    returned = lax.all_to_all(outer, REP_EP, split_axis=0, concat_axis=0, tiled=True)
    moe = mm(gates, returned)
    layer = (halves(mixed) + moe[: 2 * TOK_DEV] + moe[2 * TOK_DEV :]).astype(BF)
    layer_out = jnp.concatenate((layer[:TOK_DEV], layer[TOK_DEV:]), axis=1)
    return by_slot(served_branch), by_slot(layer_out)


def solution(mesh):
    torus = Mesh(mesh.devices.reshape(mesh.shape["rep"], 4, 4), ("rep", "ep_0", "ep_1"))

    return jax.shard_map(
        per_device,
        mesh=torus,
        in_specs=(
            P(REP_EP, None),
            P(REP_EP, None),
            P(REP_EP, None),
            P(None, EP, None),
            P(None, EP, None),
            P(REP_EP, None),
            P(None, EP, None),
            P(EP, None),
            P(REP_EP, None),
            P(REP_EP, None),
            P(),
            P(),
            P(EP, None, None),
            P(EP, None),
            P(REP_EP, None, None),
            P(REP_EP, None, None),
        ),
        out_specs=(P(REP_EP, None), P(REP_EP, None)),
        check_vma=False,
    )
```

```python
import functools

import jax
import jax.numpy as jnp
from jax import lax
from jax.experimental import pallas as pl
from jax.experimental.pallas import tpu as pltpu
from jax.sharding import Mesh
from jax.sharding import PartitionSpec as P

D = 3584
HALF = D // 2
HEADS = 64
LAT = 512
KVW = 576
VHEAD = 128
FFE = 1024
TOP = 8
PAGE = 64
SPEC = 4
REQ_DEV = 8
PAGES_DEV = 48
TOK_DEV = REQ_DEV * SPEC
N_EP = 16
HEADS_DEV = HEADS // N_EP
DEVICES = 128
CAP = 4
BAND = D // 4
EP = ("ep_0", "ep_1")
REP_EP = ("rep", "ep_0", "ep_1")
SCORE_SCALE = 192.0 ** (-0.5)
NORM_EPS = 0.25
BF = jnp.bfloat16
F32 = jnp.float32


def iota2(rows, cols, dim):
    return lax.broadcasted_iota(jnp.int32, (rows, cols), dim)


def rows_first(source_of, size=256):
    return (iota2(size, size, 1) == source_of(iota2(size, size, 0))).astype(BF)


def mm(a, b):
    return jnp.dot(a, b, preferred_element_type=F32)


def near(value):
    return pltpu.with_memory_space_constraint(value, pltpu.VMEM)


def distant(value):
    return pltpu.with_memory_space_constraint(value, pltpu.HBM)


WINDOWS = (4, 8, 12)
SPAN = 8 * KVW
LANES = 5
KEY_STEP = 49
ASK_STEP = 9


def store_lanes(ref, row, extra, value):
    count = value.shape[0]
    value = jnp.concatenate((value.astype(F32), jnp.zeros((count, LANES * 128 - KVW), F32)), axis=1)
    for tile in range(LANES):
        ref[tile, pl.ds(row + extra, count), :] = value[:, tile * 128 : tile * 128 + 128]


def load_lanes(ref, starts, stride):
    tiles = [
        jnp.concatenate([ref[tile, pl.ds(at, 8, stride=stride), :] for at in starts], axis=0)
        for tile in range(LANES)
    ]
    return jnp.concatenate([tile.astype(BF) for tile in tiles], axis=1)


def attention_body(pick_ref, count_ref, fill_ref, query_hbm, page_hbm, out_hbm, *scratch):
    key_s, query_s, page_v, query_v, out_ref, page_sem, query_sem, out_sem = scratch

    def page_load(group):
        columns = pl.ds(pl.multiple_of(group * SPAN, 128), SPAN)
        return pltpu.make_async_copy(page_hbm.at[:, columns], page_v.at[group], page_sem.at[group])

    def query_load(position, pair):
        at = position * HEADS * KVW + pair * SPAN
        return pltpu.make_async_copy(
            query_hbm.at[:, pl.ds(pl.multiple_of(at, 128), SPAN)],
            query_v.at[pair, position],
            query_sem.at[pair, position],
        )

    def result_copy(i):
        rows = pl.ds(pl.multiple_of(i * 16, 16), 16)
        return pltpu.make_async_copy(out_ref.at[:, rows], out_hbm.at[:, rows], out_sem.at[i])

    for group in range(8):
        page_load(group).start()
    for pair in range(8):
        for position in range(SPEC):
            query_load(position, pair).start()

    def spread_keys(group, carry):
        page_load(group).wait()
        for t in range(8):
            store_lanes(
                key_s,
                pl.multiple_of(group * 8 * KEY_STEP, 8),
                t * KEY_STEP,
                page_v[group, :, t * KVW : (t + 1) * KVW],
            )
        return carry

    lax.fori_loop(0, 8, spread_keys, 0)

    def spread_queries(pair, carry):
        for position in range(SPEC):
            query_load(position, pair).wait()
        for column in range(2):
            for position in range(SPEC):
                for head in range(HEADS_DEV):
                    at = (column * HEADS_DEV + head) * KVW
                    place = (column * SPEC + position) * HEADS_DEV + head
                    store_lanes(
                        query_s,
                        pl.multiple_of(pair * 32 * ASK_STEP, 8),
                        place * ASK_STEP,
                        query_v[pair, position, :, at : at + KVW],
                    )
        return carry

    lax.fori_loop(0, 8, spread_queries, 0)

    replica = lax.axis_index("rep")
    rows = SPEC * HEADS
    late = iota2(rows, 1, 0) // HEADS_DEV % SPEC - SPEC + 1

    def attend(i, offset, length, window):
        held = [pick_ref[0, jnp.minimum(offset + j, PAGES_DEV - 1)] for j in range(window)]
        keys = load_lanes(
            key_s,
            [group * 8 * KEY_STEP + page for group in range(8) for page in held],
            KEY_STEP,
        )
        asked = load_lanes(
            query_s, [block * 8 * ASK_STEP + i for block in range(rows // 8)], ASK_STEP
        )
        scores = lax.dot_general(
            asked, keys, (((1,), (1,)), ((), ())), preferred_element_type=F32
        )
        span = window * 8
        key = iota2(1, 8 * span, 1)
        token = key % span // 8 * PAGE + key // span * 8 + key % 8
        scores = jnp.where(token < late + length, scores * SCORE_SCALE, -1e30)
        exponent = jnp.exp(scores - jnp.max(scores, axis=1, keepdims=True))
        total = jnp.sum(exponent, axis=1, keepdims=True)
        latent = mm(exponent.astype(BF), keys[:, :LAT]) / total
        out_ref[:, pl.ds(pl.multiple_of(i * 16, 16), 16), :] = latent.astype(BF).reshape(
            N_EP, 16, LAT
        )

    def request(i, offset):
        count = count_ref[replica, 0, i]
        length = (count - 1) * PAGE + fill_ref[replica, 0, i]
        for least, window in zip((0,) + WINDOWS, WINDOWS):
            pl.when((count > least) & (count <= window))(
                functools.partial(attend, i, offset, length, window)
            )
        result_copy(i).start()
        return offset + count

    lax.fori_loop(0, REQ_DEV, request, jnp.int32(0))
    for i in range(REQ_DEV):
        result_copy(i).wait()


def attention(page_order, page_count, last_fill, queries, pages):
    few = pl.BlockSpec(memory_space=pltpu.SMEM)
    far = pl.BlockSpec(memory_space=pltpu.HBM)
    return pl.pallas_call(
        attention_body,
        in_specs=[few, few, few, far, far],
        out_specs=far,
        out_shape=pltpu.HBM((N_EP, REQ_DEV * 16, LAT), BF),
        scratch_shapes=[
            pltpu.VMEM((LANES, PAGE * KEY_STEP, 128), F32),
            pltpu.VMEM((LANES, SPEC * HEADS * ASK_STEP, 128), F32),
            pltpu.VMEM((8, PAGES_DEV, SPAN), BF),
            pltpu.VMEM((8, SPEC, REQ_DEV, SPAN), BF),
            pltpu.VMEM((N_EP, REQ_DEV * 16, LAT), BF),
            pltpu.SemaphoreType.DMA((8,)),
            pltpu.SemaphoreType.DMA((8, SPEC)),
            pltpu.SemaphoreType.DMA((REQ_DEV,)),
        ],
        cost_estimate=pl.CostEstimate(
            flops=7 << 30, bytes_accessed=8 << 20, transcendentals=8 * 256 * 768
        ),
        compiler_params=pltpu.CompilerParams(vmem_limit_bytes=40 << 20),
        name="attention",
    )(*[distant(each) for each in (page_order, page_count, last_fill, queries, pages)])


def weight_loads(weight_hbm, weight_ref, sems):
    loads = []
    for band in range(4):
        columns = pl.ds(band * BAND, BAND)
        loads.append(
            pltpu.make_async_copy(
                weight_hbm.at[:, columns], weight_ref.at[:, columns], sems.at[band]
            )
        )
        loads[-1].start()
    return loads


def part_of(order_ref, lifted_ref, picked_ref, weight_ref, load, band, first):
    for place in range(8):
        source = order_ref[band * N_EP + first + place]
        picked_ref[place * 32 : place * 32 + 32, :] = lifted_ref[source]
    load.wait()
    return mm(picked_ref[...], weight_ref[:, band * BAND : (band + 1) * BAND]).astype(BF)


def sent_body(order_ref, latent_ref, up_hbm, weight_hbm, *rest):
    outs, lifted_ref = rest[:4], rest[4]
    split_ref, picked_ref, part_ref, up_ref, weight_ref, in_sems, sems = rest[5:]
    up_load = pltpu.make_async_copy(up_hbm, up_ref, in_sems.at[4])
    up_load.start()
    loads = weight_loads(weight_hbm, weight_ref, in_sems)
    by_head = rows_first(
        lambda r: (r // 32 % 2) * 128 + (r % 8) * 16 + (r // 8 % 4) * 4 + r // 64
    )
    for step in range(8):
        both = mm(by_head, latent_ref[step]).astype(BF)
        for head in range(HEADS_DEV):
            split_ref[head, step * 64 : step * 64 + 64, :] = both[head * 64 : head * 64 + 64]
    up_load.wait()
    for head in range(HEADS_DEV):
        lifted = mm(split_ref[head], up_ref[head]).astype(BF)
        columns = slice(head * VHEAD, (head + 1) * VHEAD)
        lifted_ref[:, :, columns] = lifted.reshape(N_EP, 32, VHEAD)
    copies = []
    for band in range(4):
        part_ref[band] = part_of(
            order_ref, lifted_ref, picked_ref, weight_ref, loads[band], band, 8
        )
        copies.append(pltpu.make_async_copy(part_ref.at[band], outs[band], sems.at[band]))
        copies[-1].start()
    for copy in copies:
        copy.wait()


def kept_body(order_ref, lifted_ref, weight_hbm, out_ref, picked_ref, weight_ref, in_sems):
    loads = weight_loads(weight_hbm, weight_ref, in_sems)
    for band in range(4):
        out_ref[band] = part_of(
            order_ref, lifted_ref, picked_ref, weight_ref, loads[band], band, 0
        )


def project(order, latent, value_up, out_weight):
    few = pl.BlockSpec(memory_space=pltpu.SMEM)
    whole = pl.BlockSpec(memory_space=pltpu.VMEM)
    far = pl.BlockSpec(memory_space=pltpu.HBM)
    *sent, lifted = pl.pallas_call(
        sent_body,
        in_specs=[few, whole, far, far],
        out_specs=[far] * 4 + [whole],
        out_shape=[pltpu.HBM((256, BAND), BF)] * 4 + [pltpu.VMEM((N_EP, 32, 512), BF)],
        scratch_shapes=[
            pltpu.VMEM((HEADS_DEV, 512, LAT), BF),
            pltpu.VMEM((256, 512), BF),
            pltpu.VMEM((4, 256, BAND), BF),
            pltpu.VMEM((HEADS_DEV, LAT, VHEAD), BF),
            pltpu.VMEM((512, D), BF),
            pltpu.SemaphoreType.DMA((5,)),
            pltpu.SemaphoreType.DMA((4,)),
        ],
        cost_estimate=pl.CostEstimate(
            flops=2 << 30, bytes_accessed=8 << 20, transcendentals=0
        ),
        compiler_params=pltpu.CompilerParams(vmem_limit_bytes=20 << 20),
        name="project_sent",
    )(order, near(latent), distant(value_up), distant(out_weight))
    kept = pl.pallas_call(
        kept_body,
        in_specs=[few, whole, far],
        out_specs=whole,
        out_shape=pltpu.VMEM((4, 256, BAND), BF),
        scratch_shapes=[
            pltpu.VMEM((256, 512), BF),
            pltpu.VMEM((512, D), BF),
            pltpu.SemaphoreType.DMA((4,)),
        ],
        cost_estimate=pl.CostEstimate(
            flops=1 << 30, bytes_accessed=6 << 20, transcendentals=0
        ),
        compiler_params=pltpu.CompilerParams(vmem_limit_bytes=12 << 20),
        name="project_kept",
    )(order, near(lifted), distant(out_weight))
    return *sent, kept


def add_body(rows, split_at, joined, kept_ref, *rest):
    came, send, stay = rest[:split_at], rest[split_at:-1], rest[-1]
    split = 4 // split_at
    for band in range(4):
        piece = came[band // split]
        columns = slice(band % split * BAND, (band % split + 1) * BAND)
        total = kept_ref[band].astype(F32) + piece[:, columns].astype(F32)
        stay[band] = total[:rows]
        if joined:
            send[band // 2][:, band % 2 * BAND : (band % 2 + 1) * BAND] = total[rows:].astype(BF)
        else:
            send[band][...] = total[rows:].astype(BF)


def add_pieces(kept, came, joined):
    rows = kept.shape[1] // 2
    shape, count = ((rows, 2 * BAND), 2) if joined else ((rows, BAND), 4)
    whole = pl.BlockSpec(memory_space=pltpu.VMEM)
    outs = pl.pallas_call(
        functools.partial(add_body, rows, len(came), joined),
        in_specs=[whole] * (1 + len(came)),
        out_specs=[whole] * (count + 1),
        out_shape=[jax.ShapeDtypeStruct(shape, BF)] * count
        + [jax.ShapeDtypeStruct((4, rows, BAND), F32)],
        cost_estimate=pl.CostEstimate(
            flops=8 * rows * D, bytes_accessed=8 * rows * D, transcendentals=0
        ),
        compiler_params=pltpu.CompilerParams(vmem_limit_bytes=4 << 20),
        name="add_pieces",
    )(near(kept), *[near(piece) for piece in came])
    return outs[:-1], outs[-1]


def finish_body(pick_ref, kept_ref, first_ref, second_ref, own_ref, offer_ref):
    for band in range(4):
        piece = (first_ref, second_ref)[band // 2]
        columns = slice(band % 2 * BAND, (band % 2 + 1) * BAND)
        total = (kept_ref[band] + piece[:, columns].astype(F32)).astype(BF)
        own_ref[:, band * BAND : (band + 1) * BAND] = total
        offer_ref[:, band * BAND : (band + 1) * BAND] = mm(pick_ref[...], total).astype(BF)


def finish(pick, kept, first, second):
    whole = pl.BlockSpec(memory_space=pltpu.VMEM)
    return pl.pallas_call(
        finish_body,
        in_specs=[whole] * 4,
        out_specs=[whole] * 2,
        out_shape=[
            jax.ShapeDtypeStruct((TOK_DEV, D), BF),
            jax.ShapeDtypeStruct((2 * SPEC, D), BF),
        ],
        compiler_params=pltpu.CompilerParams(vmem_limit_bytes=4 << 20),
        cost_estimate=pl.CostEstimate(flops=4 << 20, bytes_accessed=1 << 20, transcendentals=0),
        name="finish",
    )(near(pick), near(kept), near(first), near(second))


def expert_body(x_ref, in_ref, out_hbm, o_hbm, x_s, h_s, o_ref, out_ref, sems, out_sem):
    loads = []
    for step in range(4):
        rows = pl.ds(step * 256, 256)
        loads.append(
            pltpu.make_async_copy(out_hbm.at[0, rows], out_ref.at[rows], out_sem.at[step])
        )
        loads[-1].start()
    apart = rows_first(lambda r: (r % 128 // 4) * 8 + (r // 128) * 4 + r % 4)
    joined = rows_first(lambda r: (r // 4 % 2) * 128 + (r // 8) * 4 + r % 4)
    for step in range(4):
        block = mm(apart, x_ref[step * 256 : step * 256 + 256, :]).astype(BF)
        x_s[step * 128 : step * 128 + 128, :HALF] = block[:128]
        x_s[step * 128 : step * 128 + 128, HALF:] = block[128:]
    for at in range(0, FFE, 256):
        value = mm(x_s[...], in_ref[0, :, at : at + 256])
        h_s[:, at : at + 256] = (value / (1.0 + jnp.exp(-value))).astype(BF)
    for load in loads:
        load.wait()
    copies = []
    for at in range(0, HALF, 256):
        halves = [
            mm(h_s[...], out_ref[:, first + at : first + at + 256]).astype(BF)
            for first in (0, HALF)
        ]
        for step in range(4):
            rows = slice(step * 128, step * 128 + 128)
            both = jnp.concatenate((halves[0][rows], halves[1][rows]), axis=0)
            o_ref[step * 256 : step * 256 + 256, at : at + 256] = mm(joined, both).astype(BF)
        copies.append(
            pltpu.make_async_copy(
                o_ref.at[:, pl.ds(at, 256)], o_hbm.at[:, pl.ds(at, 256)], sems.at[at // 256]
            )
        )
        copies[-1].start()
    for copy in copies:
        copy.wait()


def expert(incoming, expert_in, expert_out):
    whole = pl.BlockSpec(memory_space=pltpu.VMEM)
    far = pl.BlockSpec(memory_space=pltpu.HBM)
    return pl.pallas_call(
        expert_body,
        in_specs=[whole, whole, far],
        out_specs=far,
        out_shape=pltpu.HBM((DEVICES * 8, HALF), BF),
        scratch_shapes=[
            pltpu.VMEM((512, D), BF),
            pltpu.VMEM((512, FFE), BF),
            pltpu.VMEM((DEVICES * 8, HALF), BF),
            pltpu.VMEM((FFE, D), BF),
            pltpu.SemaphoreType.DMA((7,)),
            pltpu.SemaphoreType.DMA((4,)),
        ],
        cost_estimate=pl.CostEstimate(
            flops=8 << 30, bytes_accessed=22 << 20, transcendentals=512 * 1024
        ),
        compiler_params=pltpu.CompilerParams(vmem_limit_bytes=32 << 20),
        name="expert",
    )(near(incoming), near(expert_in), distant(expert_out))


NEAR = [(0, 1), (1, 0), (2, 3), (3, 2)]
FAR = [(0, 3), (3, 0), (1, 2), (2, 1)]
PAIRS = {1: NEAR, 3: FAR}
ROUTES = (
    (("ep_0", 1), ("ep_0", 3), ("ep_1", 1), ("ep_1", 3)),
    (("ep_0", 3), ("ep_0", 1), ("ep_1", 1), ("ep_1", 3)),
    (("ep_1", 1), ("ep_1", 3), ("ep_0", 1), ("ep_0", 3)),
    (("ep_1", 3), ("ep_1", 1), ("ep_0", 1), ("ep_0", 3)),
)


def block_order():
    first, second = [], []
    for route in ROUTES:
        places = [(0, 0)]
        for axis, flip in reversed(route):
            turn = (flip, 0) if axis == "ep_0" else (0, flip)
            places = places + [(a ^ turn[0], b ^ turn[1]) for a, b in places]
        first += [a for a, _ in places]
        second += [b for _, b in places]
    mine = lax.axis_index("ep_0"), lax.axis_index("ep_1")
    return (jnp.array(first, jnp.int32) ^ mine[0]) * 4 + (jnp.array(second, jnp.int32) ^ mine[1])


def exchange(pieces, step):
    every = 4 // len(pieces)
    out = []
    for at, piece in enumerate(pieces):
        axis, flip = ROUTES[at * every][step]
        out.append(lax.ppermute(piece, axis, PAIRS[flip]))
    return out


def sum_over_columns(pick, parts):
    *send, kept = parts
    for step in range(3):
        send, kept = add_pieces(kept, exchange(send, step), joined=step > 0)
    return finish(pick, kept, *exchange(send, 3))


def shifted(value, axis, steps):
    count = lax.axis_size(axis)
    return lax.ppermute(value, axis, [(s, (s + steps) % count) for s in range(count)])


def from_replicas(value, odd):
    crossed = lax.ppermute(value, "rep", [(i, i ^ 1) for i in range(8)])
    value = jnp.where(odd, crossed, value)
    planes = [shifted(value, "rep", 2 * back) for back in range(1, 4)]
    return jnp.concatenate([value] + planes, axis=0)


def by_position(value):
    return jnp.concatenate([value[:, s * D : (s + 1) * D] for s in range(SPEC)], axis=0)


def by_slot(value):
    return jnp.concatenate([value[s * REQ_DEV : (s + 1) * REQ_DEV] for s in range(SPEC)], axis=1)


def per_device(
    latent_pages,
    queries,
    residual,
    page_count,
    last_fill,
    page_order,
    shed_slots,
    shed_shift,
    expert_ids,
    gate_weight,
    expert_home,
    norm_gain,
    value_up,
    out_weight,
    expert_in,
    expert_out,
):
    replica = lax.axis_index("rep")
    latent = attention(page_order, page_count, last_fill, queries, latent_pages)
    latent = lax.all_to_all(latent, EP, split_axis=0, concat_axis=0, tiled=True)
    tokens = jnp.arange(TOK_DEV, dtype=jnp.int32)
    own_sheds = shed_slots[replica, 0, :]
    shed_rows = (jnp.arange(SPEC, dtype=jnp.int32) * REQ_DEV + own_sheds[:, None]).reshape(-1)
    pick = shed_rows[:, None] == tokens[None, :]
    present = jnp.any(pick, axis=0)[:, None]
    row_shifts = jnp.repeat(shed_shift[0], SPEC)
    odd = (row_shifts % 2 == 1)[:, None]
    planes = (row_shifts + 1 - replica % 2) // 2 % 4
    wanted = jnp.arange(4, dtype=jnp.int32)[:, None] == planes[None, :]
    place = (wanted[:, :, None] & pick[None, :, :]).reshape(4 * 2 * SPEC, TOK_DEV).astype(BF)
    pick = pick.astype(BF)

    def served(own, came):
        taken = lax.dot_general(place, came, (((0,), (0,)), ((), ())), preferred_element_type=F32)
        return jnp.where(present, taken.astype(BF), own)

    own_residual = by_position(residual)
    came = from_replicas(mm(pick, own_residual).astype(BF), odd)
    latent, came = lax.optimization_barrier((latent, came))
    served_residual = served(own_residual, came)
    own_branch, offer = sum_over_columns(
        pick, project(block_order(), latent.reshape(8, 256, LAT), value_up, out_weight)
    )
    served_branch = served(own_branch, from_replicas(offer, odd))
    mixed = served_residual.astype(F32) + served_branch.astype(F32)
    square = jnp.mean(mixed * mixed, axis=1, keepdims=True)
    normed = (mixed * lax.rsqrt(square + NORM_EPS) * norm_gain).astype(BF)

    def routed(value):
        return value.reshape(REQ_DEV, SPEC, TOP).transpose(1, 0, 2).reshape(TOK_DEV, TOP)

    gate_weight = routed(gate_weight)
    target = expert_home[routed(expert_ids).reshape(-1)]
    hits = (target[:, None] == jnp.arange(DEVICES, dtype=jnp.int32)[None, :]).astype(jnp.int32)
    before = jnp.sum((jnp.cumsum(hits, axis=0) - hits) * hits, axis=1)
    slot = (target * CAP + before).reshape(TOK_DEV, TOP)
    row = jnp.arange(DEVICES * 8, dtype=jnp.int32)
    row_slot = row // 8 * CAP + row % CAP
    row_half = row // CAP % 2
    both = jnp.arange(2 * TOK_DEV, dtype=jnp.int32)
    same_half = row_half[None, :] == (both // TOK_DEV)[:, None]
    landing = slot[:, :, None] == row_slot[None, None, :]
    chosen = jnp.any(landing, axis=1)
    chooser = (jnp.concatenate((chosen, chosen)) & same_half).astype(BF)
    gates = jnp.sum(jnp.where(landing, gate_weight[:, :, None], 0.0), axis=1)
    gates = jnp.where(same_half, jnp.concatenate((gates, gates)), 0.0)
    coarse = lax.reduce_precision(gates, 8, 7)
    gates = jnp.concatenate((coarse.astype(BF), (gates - coarse).astype(BF)))

    def halves(value):
        return jnp.concatenate((value[:, :HALF], value[:, HALF:]), axis=0)

    outgoing = lax.dot_general(
        chooser, halves(normed), (((0,), (0,)), ((), ())), preferred_element_type=F32
    ).astype(BF)
    incoming = lax.all_to_all(outgoing, REP_EP, split_axis=0, concat_axis=0, tiled=True)
    outer = expert(incoming, expert_in, expert_out)
    returned = lax.all_to_all(outer, REP_EP, split_axis=0, concat_axis=0, tiled=True)
    moe = mm(gates, returned)
    layer = (halves(mixed) + moe[: 2 * TOK_DEV] + moe[2 * TOK_DEV :]).astype(BF)
    layer_out = jnp.concatenate((layer[:TOK_DEV], layer[TOK_DEV:]), axis=1)
    return by_slot(served_branch), by_slot(layer_out)


def solution(mesh):
    torus = Mesh(mesh.devices.reshape(mesh.shape["rep"], 4, 4), ("rep", "ep_0", "ep_1"))

    return jax.shard_map(
        per_device,
        mesh=torus,
        in_specs=(
            P(REP_EP, None),
            P(REP_EP, None),
            P(REP_EP, None),
            P(None, EP, None),
            P(None, EP, None),
            P(REP_EP, None),
            P(None, EP, None),
            P(EP, None),
            P(REP_EP, None),
            P(REP_EP, None),
            P(),
            P(),
            P(EP, None, None),
            P(EP, None),
            P(REP_EP, None, None),
            P(REP_EP, None, None),
        ),
        out_specs=(P(REP_EP, None), P(REP_EP, None)),
        check_vma=False,
    )
```

```python
import functools

import jax
import jax.numpy as jnp
from jax import lax
from jax.experimental import pallas as pl
from jax.experimental.pallas import tpu as pltpu
from jax.sharding import Mesh
from jax.sharding import PartitionSpec as P

D = 3584
HALF = D // 2
HEADS = 64
LAT = 512
KVW = 576
VHEAD = 128
FFE = 1024
TOP = 8
PAGE = 64
SPEC = 4
REQ_DEV = 8
PAGES_DEV = 48
TOK_DEV = REQ_DEV * SPEC
N_EP = 16
HEADS_DEV = HEADS // N_EP
DEVICES = 128
CAP = 4
BAND = D // 4
EP = ("ep_0", "ep_1")
REP_EP = ("rep", "ep_0", "ep_1")
SCORE_SCALE = 192.0 ** (-0.5)
NORM_EPS = 0.25
BF = jnp.bfloat16
F32 = jnp.float32


def iota2(rows, cols, dim):
    return lax.broadcasted_iota(jnp.int32, (rows, cols), dim)


def rows_first(source_of, size=256):
    return (iota2(size, size, 1) == source_of(iota2(size, size, 0))).astype(BF)


def mm(a, b):
    return jnp.dot(a, b, preferred_element_type=F32)


def near(value):
    return pltpu.with_memory_space_constraint(value, pltpu.VMEM)


def distant(value):
    return pltpu.with_memory_space_constraint(value, pltpu.HBM)


WINDOWS = (4, 8, 12)
SPAN = 8 * KVW
LANES = 5
KEY_STEP = 49
ASK_STEP = 9


def store_lanes(ref, row, extra, value):
    count = value.shape[0]
    value = jnp.concatenate((value.astype(F32), jnp.zeros((count, LANES * 128 - KVW), F32)), axis=1)
    for tile in range(LANES):
        ref[tile, pl.ds(row + extra, count), :] = value[:, tile * 128 : tile * 128 + 128]


def load_lanes(ref, starts, stride):
    tiles = [
        jnp.concatenate([ref[tile, pl.ds(at, 8, stride=stride), :] for at in starts], axis=0)
        for tile in range(LANES)
    ]
    return jnp.concatenate([tile.astype(BF) for tile in tiles], axis=1)


def attention_body(pick_ref, count_ref, fill_ref, query_hbm, page_hbm, out_hbm, *scratch):
    key_s, query_s, page_v, query_v, out_ref, page_sem, query_sem, out_sem = scratch

    def page_load(group):
        columns = pl.ds(pl.multiple_of(group * SPAN, 128), SPAN)
        return pltpu.make_async_copy(page_hbm.at[:, columns], page_v.at[group], page_sem.at[group])

    def query_load(position, pair):
        at = position * HEADS * KVW + pair * SPAN
        return pltpu.make_async_copy(
            query_hbm.at[:, pl.ds(pl.multiple_of(at, 128), SPAN)],
            query_v.at[pair, position],
            query_sem.at[pair, position],
        )

    def result_copy(i):
        rows = pl.ds(pl.multiple_of(i * 16, 16), 16)
        return pltpu.make_async_copy(out_ref.at[:, rows], out_hbm.at[:, rows], out_sem.at[i])

    for group in range(8):
        page_load(group).start()
    for pair in range(8):
        for position in range(SPEC):
            query_load(position, pair).start()

    def spread_keys(group, carry):
        page_load(group).wait()
        for t in range(8):
            store_lanes(
                key_s,
                pl.multiple_of(group * 8 * KEY_STEP, 8),
                t * KEY_STEP,
                page_v[group, :, t * KVW : (t + 1) * KVW],
            )
        return carry

    lax.fori_loop(0, 8, spread_keys, 0)

    def spread_queries(pair, carry):
        for position in range(SPEC):
            query_load(position, pair).wait()
        for column in range(2):
            for position in range(SPEC):
                for head in range(HEADS_DEV):
                    at = (column * HEADS_DEV + head) * KVW
                    place = (column * SPEC + position) * HEADS_DEV + head
                    store_lanes(
                        query_s,
                        pl.multiple_of(pair * 32 * ASK_STEP, 8),
                        place * ASK_STEP,
                        query_v[pair, position, :, at : at + KVW],
                    )
        return carry

    lax.fori_loop(0, 8, spread_queries, 0)

    replica = lax.axis_index("rep")
    rows = SPEC * HEADS
    late = iota2(rows, 1, 0) // HEADS_DEV % SPEC - SPEC + 1

    def attend(i, offset, length, window):
        held = [pick_ref[0, jnp.minimum(offset + j, PAGES_DEV - 1)] for j in range(window)]
        keys = load_lanes(
            key_s,
            [group * 8 * KEY_STEP + page for group in range(8) for page in held],
            KEY_STEP,
        )
        asked = load_lanes(
            query_s, [block * 8 * ASK_STEP + i for block in range(rows // 8)], ASK_STEP
        )
        scores = lax.dot_general(
            asked, keys, (((1,), (1,)), ((), ())), preferred_element_type=F32
        )
        span = window * 8
        key = iota2(1, 8 * span, 1)
        token = key % span // 8 * PAGE + key // span * 8 + key % 8
        scores = jnp.where(token < late + length, scores * SCORE_SCALE, -1e30)
        exponent = jnp.exp(scores - jnp.max(scores, axis=1, keepdims=True))
        total = jnp.sum(exponent, axis=1, keepdims=True)
        latent = mm(exponent.astype(BF), keys[:, :LAT]) / total
        out_ref[:, pl.ds(pl.multiple_of(i * 16, 16), 16), :] = latent.astype(BF).reshape(
            N_EP, 16, LAT
        )

    def request(i, offset):
        count = count_ref[replica, 0, i]
        length = (count - 1) * PAGE + fill_ref[replica, 0, i]
        for least, window in zip((0,) + WINDOWS, WINDOWS):
            pl.when((count > least) & (count <= window))(
                functools.partial(attend, i, offset, length, window)
            )
        result_copy(i).start()
        return offset + count

    lax.fori_loop(0, REQ_DEV, request, jnp.int32(0))
    for i in range(REQ_DEV):
        result_copy(i).wait()


def attention(page_order, page_count, last_fill, queries, pages):
    few = pl.BlockSpec(memory_space=pltpu.SMEM)
    far = pl.BlockSpec(memory_space=pltpu.HBM)
    return pl.pallas_call(
        attention_body,
        in_specs=[few, few, few, far, far],
        out_specs=far,
        out_shape=pltpu.HBM((N_EP, REQ_DEV * 16, LAT), BF),
        scratch_shapes=[
            pltpu.VMEM((LANES, PAGE * KEY_STEP, 128), F32),
            pltpu.VMEM((LANES, SPEC * HEADS * ASK_STEP, 128), F32),
            pltpu.VMEM((8, PAGES_DEV, SPAN), BF),
            pltpu.VMEM((8, SPEC, REQ_DEV, SPAN), BF),
            pltpu.VMEM((N_EP, REQ_DEV * 16, LAT), BF),
            pltpu.SemaphoreType.DMA((8,)),
            pltpu.SemaphoreType.DMA((8, SPEC)),
            pltpu.SemaphoreType.DMA((REQ_DEV,)),
        ],
        cost_estimate=pl.CostEstimate(
            flops=7 << 30, bytes_accessed=8 << 20, transcendentals=8 * 256 * 768
        ),
        compiler_params=pltpu.CompilerParams(vmem_limit_bytes=40 << 20),
        name="attention",
    )(*[distant(each) for each in (page_order, page_count, last_fill, queries, pages)])


def weight_loads(weight_hbm, weight_ref, sems):
    loads = []
    for band in range(4):
        columns = pl.ds(band * BAND, BAND)
        loads.append(
            pltpu.make_async_copy(
                weight_hbm.at[:, columns], weight_ref.at[:, columns], sems.at[band]
            )
        )
        loads[-1].start()
    return loads


def part_of(order_ref, lifted_ref, picked_ref, weight_ref, load, band, first):
    for place in range(8):
        source = order_ref[band * N_EP + first + place]
        picked_ref[place * 32 : place * 32 + 32, :] = lifted_ref[source]
    load.wait()
    return mm(picked_ref[...], weight_ref[:, band * BAND : (band + 1) * BAND]).astype(BF)


def sent_body(order_ref, latent_ref, up_hbm, weight_hbm, *rest):
    outs, lifted_ref = rest[:4], rest[4]
    split_ref, picked_ref, part_ref, up_ref, weight_ref, in_sems, sems = rest[5:]
    up_load = pltpu.make_async_copy(up_hbm, up_ref, in_sems.at[4])
    up_load.start()
    loads = weight_loads(weight_hbm, weight_ref, in_sems)
    by_head = rows_first(
        lambda r: (r // 32 % 2) * 128 + (r % 8) * 16 + (r // 8 % 4) * 4 + r // 64
    )

    def split(turn, carry):
        for part in range(4):
            step = turn * 4 + part
            both = mm(by_head, latent_ref[step]).astype(BF)
            at = pl.multiple_of(step * 64, 64)
            for head in range(HEADS_DEV):
                split_ref[head, pl.ds(at, 64), :] = both[head * 64 : head * 64 + 64]
        return carry

    lax.fori_loop(0, 2, split, 0)
    up_load.wait()
    for head in range(HEADS_DEV):
        lifted = mm(split_ref[head], up_ref[head]).astype(BF)
        columns = slice(head * VHEAD, (head + 1) * VHEAD)
        lifted_ref[:, :, columns] = lifted.reshape(N_EP, 32, VHEAD)
    copies = []
    for band in range(4):
        part_ref[band] = part_of(
            order_ref, lifted_ref, picked_ref, weight_ref, loads[band], band, 8
        )
        copies.append(pltpu.make_async_copy(part_ref.at[band], outs[band], sems.at[band]))
        copies[-1].start()
    for copy in copies:
        copy.wait()


def kept_body(order_ref, lifted_ref, weight_hbm, out_ref, picked_ref, weight_ref, in_sems):
    loads = weight_loads(weight_hbm, weight_ref, in_sems)
    for band in range(4):
        out_ref[band] = part_of(
            order_ref, lifted_ref, picked_ref, weight_ref, loads[band], band, 0
        )


def project(order, latent, value_up, out_weight):
    few = pl.BlockSpec(memory_space=pltpu.SMEM)
    whole = pl.BlockSpec(memory_space=pltpu.VMEM)
    far = pl.BlockSpec(memory_space=pltpu.HBM)
    *sent, lifted = pl.pallas_call(
        sent_body,
        in_specs=[few, whole, far, far],
        out_specs=[far] * 4 + [whole],
        out_shape=[pltpu.HBM((256, BAND), BF)] * 4 + [pltpu.VMEM((N_EP, 32, 512), BF)],
        scratch_shapes=[
            pltpu.VMEM((HEADS_DEV, 512, LAT), BF),
            pltpu.VMEM((256, 512), BF),
            pltpu.VMEM((4, 256, BAND), BF),
            pltpu.VMEM((HEADS_DEV, LAT, VHEAD), BF),
            pltpu.VMEM((512, D), BF),
            pltpu.SemaphoreType.DMA((5,)),
            pltpu.SemaphoreType.DMA((4,)),
        ],
        cost_estimate=pl.CostEstimate(
            flops=2 << 30, bytes_accessed=8 << 20, transcendentals=0
        ),
        compiler_params=pltpu.CompilerParams(vmem_limit_bytes=20 << 20),
        name="project_sent",
    )(order, near(latent), distant(value_up), distant(out_weight))
    kept = pl.pallas_call(
        kept_body,
        in_specs=[few, whole, far],
        out_specs=whole,
        out_shape=pltpu.VMEM((4, 256, BAND), BF),
        scratch_shapes=[
            pltpu.VMEM((256, 512), BF),
            pltpu.VMEM((512, D), BF),
            pltpu.SemaphoreType.DMA((4,)),
        ],
        cost_estimate=pl.CostEstimate(
            flops=1 << 30, bytes_accessed=6 << 20, transcendentals=0
        ),
        compiler_params=pltpu.CompilerParams(vmem_limit_bytes=12 << 20),
        name="project_kept",
    )(order, near(lifted), distant(out_weight))
    return *sent, kept


def add_body(rows, split_at, joined, kept_ref, *rest):
    came, send, stay = rest[:split_at], rest[split_at:-1], rest[-1]
    split = 4 // split_at
    for band in range(4):
        piece = came[band // split]
        columns = slice(band % split * BAND, (band % split + 1) * BAND)
        total = kept_ref[band].astype(F32) + piece[:, columns].astype(F32)
        stay[band] = total[:rows]
        if joined:
            send[band // 2][:, band % 2 * BAND : (band % 2 + 1) * BAND] = total[rows:].astype(BF)
        else:
            send[band][...] = total[rows:].astype(BF)


def add_pieces(kept, came, joined):
    rows = kept.shape[1] // 2
    shape, count = ((rows, 2 * BAND), 2) if joined else ((rows, BAND), 4)
    whole = pl.BlockSpec(memory_space=pltpu.VMEM)
    outs = pl.pallas_call(
        functools.partial(add_body, rows, len(came), joined),
        in_specs=[whole] * (1 + len(came)),
        out_specs=[whole] * (count + 1),
        out_shape=[jax.ShapeDtypeStruct(shape, BF)] * count
        + [jax.ShapeDtypeStruct((4, rows, BAND), F32)],
        cost_estimate=pl.CostEstimate(
            flops=8 * rows * D, bytes_accessed=8 * rows * D, transcendentals=0
        ),
        compiler_params=pltpu.CompilerParams(vmem_limit_bytes=4 << 20),
        name="add_pieces",
    )(near(kept), *[near(piece) for piece in came])
    return outs[:-1], outs[-1]


def finish_body(pick_ref, kept_ref, first_ref, second_ref, own_ref, offer_ref):
    for band in range(4):
        piece = (first_ref, second_ref)[band // 2]
        columns = slice(band % 2 * BAND, (band % 2 + 1) * BAND)
        total = (kept_ref[band] + piece[:, columns].astype(F32)).astype(BF)
        own_ref[:, band * BAND : (band + 1) * BAND] = total
        offer_ref[:, band * BAND : (band + 1) * BAND] = mm(pick_ref[...], total).astype(BF)


def finish(pick, kept, first, second):
    whole = pl.BlockSpec(memory_space=pltpu.VMEM)
    return pl.pallas_call(
        finish_body,
        in_specs=[whole] * 4,
        out_specs=[whole] * 2,
        out_shape=[
            jax.ShapeDtypeStruct((TOK_DEV, D), BF),
            jax.ShapeDtypeStruct((2 * SPEC, D), BF),
        ],
        compiler_params=pltpu.CompilerParams(vmem_limit_bytes=4 << 20),
        cost_estimate=pl.CostEstimate(flops=4 << 20, bytes_accessed=1 << 20, transcendentals=0),
        name="finish",
    )(near(pick), near(kept), near(first), near(second))


def expert_body(x_ref, in_ref, out_hbm, o_hbm, x_s, h_s, o_ref, out_ref, sems, out_sem):
    loads = [pltpu.make_async_copy(out_hbm.at[0], out_ref, out_sem.at[0])]
    loads[0].start()
    apart = rows_first(lambda r: (r % 128 // 4) * 8 + (r // 128) * 4 + r % 4)
    joined = rows_first(lambda r: (r // 4 % 2) * 128 + (r // 8) * 4 + r % 4)
    for step in range(4):
        block = mm(apart, x_ref[step * 256 : step * 256 + 256, :]).astype(BF)
        x_s[step * 128 : step * 128 + 128, :HALF] = block[:128]
        x_s[step * 128 : step * 128 + 128, HALF:] = block[128:]

    def inner(step, carry):
        columns = pl.ds(pl.multiple_of(step * 512, 512), 512)
        value = mm(x_s[...], in_ref[0, :, columns])
        h_s[:, columns] = (value / (1.0 + jnp.exp(-value))).astype(BF)
        return carry

    lax.fori_loop(0, 2, inner, 0)
    for load in loads:
        load.wait()
    copies = []
    for at in range(0, HALF, 256):
        halves = [
            mm(h_s[...], out_ref[:, first + at : first + at + 256]).astype(BF)
            for first in (0, HALF)
        ]
        for step in range(4):
            rows = slice(step * 128, step * 128 + 128)
            both = jnp.concatenate((halves[0][rows], halves[1][rows]), axis=0)
            o_ref[step * 256 : step * 256 + 256, at : at + 256] = mm(joined, both).astype(BF)
        copies.append(
            pltpu.make_async_copy(
                o_ref.at[:, pl.ds(at, 256)], o_hbm.at[:, pl.ds(at, 256)], sems.at[at // 256]
            )
        )
        copies[-1].start()
    for copy in copies:
        copy.wait()


def expert(incoming, expert_in, expert_out):
    whole = pl.BlockSpec(memory_space=pltpu.VMEM)
    far = pl.BlockSpec(memory_space=pltpu.HBM)
    return pl.pallas_call(
        expert_body,
        in_specs=[whole, whole, far],
        out_specs=far,
        out_shape=pltpu.HBM((DEVICES * 8, HALF), BF),
        scratch_shapes=[
            pltpu.VMEM((512, D), BF),
            pltpu.VMEM((512, FFE), BF),
            pltpu.VMEM((DEVICES * 8, HALF), BF),
            pltpu.VMEM((FFE, D), BF),
            pltpu.SemaphoreType.DMA((7,)),
            pltpu.SemaphoreType.DMA((4,)),
        ],
        cost_estimate=pl.CostEstimate(
            flops=8 << 30, bytes_accessed=22 << 20, transcendentals=512 * 1024
        ),
        compiler_params=pltpu.CompilerParams(vmem_limit_bytes=32 << 20),
        name="expert",
    )(near(incoming), near(expert_in), distant(expert_out))


NEAR = [(0, 1), (1, 0), (2, 3), (3, 2)]
FAR = [(0, 3), (3, 0), (1, 2), (2, 1)]
PAIRS = {1: NEAR, 3: FAR}
ROUTES = (
    (("ep_0", 1), ("ep_0", 3), ("ep_1", 1), ("ep_1", 3)),
    (("ep_0", 3), ("ep_0", 1), ("ep_1", 1), ("ep_1", 3)),
    (("ep_1", 1), ("ep_1", 3), ("ep_0", 1), ("ep_0", 3)),
    (("ep_1", 3), ("ep_1", 1), ("ep_0", 1), ("ep_0", 3)),
)


def block_order():
    first, second = [], []
    for route in ROUTES:
        places = [(0, 0)]
        for axis, flip in reversed(route):
            turn = (flip, 0) if axis == "ep_0" else (0, flip)
            places = places + [(a ^ turn[0], b ^ turn[1]) for a, b in places]
        first += [a for a, _ in places]
        second += [b for _, b in places]
    mine = lax.axis_index("ep_0"), lax.axis_index("ep_1")
    return (jnp.array(first, jnp.int32) ^ mine[0]) * 4 + (jnp.array(second, jnp.int32) ^ mine[1])


def exchange(pieces, step):
    every = 4 // len(pieces)
    out = []
    for at, piece in enumerate(pieces):
        axis, flip = ROUTES[at * every][step]
        out.append(lax.ppermute(piece, axis, PAIRS[flip]))
    return out


def sum_over_columns(pick, parts):
    *send, kept = parts
    for step in range(3):
        send, kept = add_pieces(kept, exchange(send, step), joined=step > 0)
    return finish(pick, kept, *exchange(send, 3))


def shifted(value, axis, steps):
    count = lax.axis_size(axis)
    return lax.ppermute(value, axis, [(s, (s + steps) % count) for s in range(count)])


def from_replicas(value, odd):
    crossed = lax.ppermute(value, "rep", [(i, i ^ 1) for i in range(8)])
    value = jnp.where(odd, crossed, value)
    planes = [shifted(value, "rep", 2 * back) for back in range(1, 4)]
    return jnp.concatenate([value] + planes, axis=0)


def by_position(value):
    return jnp.concatenate([value[:, s * D : (s + 1) * D] for s in range(SPEC)], axis=0)


def by_slot(value):
    return jnp.concatenate([value[s * REQ_DEV : (s + 1) * REQ_DEV] for s in range(SPEC)], axis=1)


def per_device(
    latent_pages,
    queries,
    residual,
    page_count,
    last_fill,
    page_order,
    shed_slots,
    shed_shift,
    expert_ids,
    gate_weight,
    expert_home,
    norm_gain,
    value_up,
    out_weight,
    expert_in,
    expert_out,
):
    replica = lax.axis_index("rep")
    latent = attention(page_order, page_count, last_fill, queries, latent_pages)
    latent = lax.all_to_all(latent, EP, split_axis=0, concat_axis=0, tiled=True)
    tokens = jnp.arange(TOK_DEV, dtype=jnp.int32)
    own_sheds = shed_slots[replica, 0, :]
    shed_rows = (jnp.arange(SPEC, dtype=jnp.int32) * REQ_DEV + own_sheds[:, None]).reshape(-1)
    pick = shed_rows[:, None] == tokens[None, :]
    present = jnp.any(pick, axis=0)[:, None]
    row_shifts = jnp.repeat(shed_shift[0], SPEC)
    odd = (row_shifts % 2 == 1)[:, None]
    planes = (row_shifts + 1 - replica % 2) // 2 % 4
    wanted = jnp.arange(4, dtype=jnp.int32)[:, None] == planes[None, :]
    place = (wanted[:, :, None] & pick[None, :, :]).reshape(4 * 2 * SPEC, TOK_DEV).astype(BF)
    pick = pick.astype(BF)

    def served(own, came):
        taken = lax.dot_general(place, came, (((0,), (0,)), ((), ())), preferred_element_type=F32)
        return jnp.where(present, taken.astype(BF), own)

    own_residual = by_position(residual)
    came = from_replicas(mm(pick, own_residual).astype(BF), odd)
    latent, came = lax.optimization_barrier((latent, came))
    served_residual = served(own_residual, came)
    own_branch, offer = sum_over_columns(
        pick, project(block_order(), latent.reshape(8, 256, LAT), value_up, out_weight)
    )
    served_branch = served(own_branch, from_replicas(offer, odd))
    mixed = served_residual.astype(F32) + served_branch.astype(F32)
    square = jnp.mean(mixed * mixed, axis=1, keepdims=True)
    normed = (mixed * lax.rsqrt(square + NORM_EPS) * norm_gain).astype(BF)

    def routed(value):
        return value.reshape(REQ_DEV, SPEC, TOP).transpose(1, 0, 2).reshape(TOK_DEV, TOP)

    gate_weight = routed(gate_weight)
    target = expert_home[routed(expert_ids).reshape(-1)]
    hits = (target[:, None] == jnp.arange(DEVICES, dtype=jnp.int32)[None, :]).astype(jnp.int32)
    before = jnp.sum((jnp.cumsum(hits, axis=0) - hits) * hits, axis=1)
    slot = (target * CAP + before).reshape(TOK_DEV, TOP)
    row = jnp.arange(DEVICES * 8, dtype=jnp.int32)
    row_slot = row // 8 * CAP + row % CAP
    row_half = row // CAP % 2
    both = jnp.arange(2 * TOK_DEV, dtype=jnp.int32)
    same_half = row_half[None, :] == (both // TOK_DEV)[:, None]
    landing = slot[:, :, None] == row_slot[None, None, :]
    chosen = jnp.any(landing, axis=1)
    chooser = (jnp.concatenate((chosen, chosen)) & same_half).astype(BF)
    gates = jnp.sum(jnp.where(landing, gate_weight[:, :, None], 0.0), axis=1)
    gates = jnp.where(same_half, jnp.concatenate((gates, gates)), 0.0)
    coarse = lax.reduce_precision(gates, 8, 7)
    gates = jnp.concatenate((coarse.astype(BF), (gates - coarse).astype(BF)))

    def halves(value):
        return jnp.concatenate((value[:, :HALF], value[:, HALF:]), axis=0)

    outgoing = lax.dot_general(
        chooser, halves(normed), (((0,), (0,)), ((), ())), preferred_element_type=F32
    ).astype(BF)
    incoming = lax.all_to_all(outgoing, REP_EP, split_axis=0, concat_axis=0, tiled=True)
    outer = expert(incoming, expert_in, expert_out)
    returned = lax.all_to_all(outer, REP_EP, split_axis=0, concat_axis=0, tiled=True)
    moe = mm(gates, returned)
    layer = (halves(mixed) + moe[: 2 * TOK_DEV] + moe[2 * TOK_DEV :]).astype(BF)
    layer_out = jnp.concatenate((layer[:TOK_DEV], layer[TOK_DEV:]), axis=1)
    return by_slot(served_branch), by_slot(layer_out)


def solution(mesh):
    torus = Mesh(mesh.devices.reshape(mesh.shape["rep"], 4, 4), ("rep", "ep_0", "ep_1"))

    return jax.shard_map(
        per_device,
        mesh=torus,
        in_specs=(
            P(REP_EP, None),
            P(REP_EP, None),
            P(REP_EP, None),
            P(None, EP, None),
            P(None, EP, None),
            P(REP_EP, None),
            P(None, EP, None),
            P(EP, None),
            P(REP_EP, None),
            P(REP_EP, None),
            P(),
            P(),
            P(EP, None, None),
            P(EP, None),
            P(REP_EP, None, None),
            P(REP_EP, None, None),
        ),
        out_specs=(P(REP_EP, None), P(REP_EP, None)),
        check_vma=False,
    )
```

```python
import functools

import jax
import jax.numpy as jnp
from jax import lax
from jax.experimental import pallas as pl
from jax.experimental.pallas import tpu as pltpu
from jax.sharding import Mesh
from jax.sharding import PartitionSpec as P

D = 3584
HALF = D // 2
HEADS = 64
LAT = 512
KVW = 576
VHEAD = 128
FFE = 1024
TOP = 8
PAGE = 64
SPEC = 4
REQ_DEV = 8
PAGES_DEV = 48
TOK_DEV = REQ_DEV * SPEC
N_EP = 16
HEADS_DEV = HEADS // N_EP
DEVICES = 128
CAP = 4
BAND = D // 4
EP = ("ep_0", "ep_1")
REP_EP = ("rep", "ep_0", "ep_1")
SCORE_SCALE = 192.0 ** (-0.5)
NORM_EPS = 0.25
BF = jnp.bfloat16
F32 = jnp.float32


def iota2(rows, cols, dim):
    return lax.broadcasted_iota(jnp.int32, (rows, cols), dim)


def rows_first(source_of, size=256):
    return (iota2(size, size, 1) == source_of(iota2(size, size, 0))).astype(BF)


def mm(a, b):
    return jnp.dot(a, b, preferred_element_type=F32)


def near(value):
    return pltpu.with_memory_space_constraint(value, pltpu.VMEM)


def distant(value):
    return pltpu.with_memory_space_constraint(value, pltpu.HBM)


WINDOWS = (4, 8, 12)
SPAN = 8 * KVW
LANES = 5
KEY_STEP = 49
ASK_STEP = 9


def store_lanes(ref, row, extra, value):
    count = value.shape[0]
    value = jnp.concatenate((value.astype(F32), jnp.zeros((count, LANES * 128 - KVW), F32)), axis=1)
    for tile in range(LANES):
        ref[tile, pl.ds(row + extra, count), :] = value[:, tile * 128 : tile * 128 + 128]


def load_lanes(ref, starts, stride):
    tiles = [
        jnp.concatenate([ref[tile, pl.ds(at, 8, stride=stride), :] for at in starts], axis=0)
        for tile in range(LANES)
    ]
    return jnp.concatenate([tile.astype(BF) for tile in tiles], axis=1)


def attention_body(pick_ref, count_ref, fill_ref, query_hbm, page_hbm, out_hbm, *scratch):
    key_s, query_s, page_v, query_v, out_ref, page_sem, query_sem, out_sem = scratch

    def page_load(group):
        columns = pl.ds(pl.multiple_of(group * SPAN, 128), SPAN)
        return pltpu.make_async_copy(page_hbm.at[:, columns], page_v.at[group], page_sem.at[group])

    def query_load(position, pair):
        at = position * HEADS * KVW + pair * SPAN
        return pltpu.make_async_copy(
            query_hbm.at[:, pl.ds(pl.multiple_of(at, 128), SPAN)],
            query_v.at[pair, position],
            query_sem.at[pair, position],
        )

    def result_copy(i):
        rows = pl.ds(pl.multiple_of(i * 16, 16), 16)
        return pltpu.make_async_copy(out_ref.at[:, rows], out_hbm.at[:, rows], out_sem.at[i])

    for group in range(8):
        page_load(group).start()
    for pair in range(8):
        for position in range(SPEC):
            query_load(position, pair).start()

    def spread_keys(group, carry):
        page_load(group).wait()
        for t in range(8):
            store_lanes(
                key_s,
                pl.multiple_of(group * 8 * KEY_STEP, 8),
                t * KEY_STEP,
                page_v[group, :, t * KVW : (t + 1) * KVW],
            )
        return carry

    lax.fori_loop(0, 8, spread_keys, 0)

    def spread_queries(pair, carry):
        for position in range(SPEC):
            query_load(position, pair).wait()
        for column in range(2):
            for position in range(SPEC):
                for head in range(HEADS_DEV):
                    at = (column * HEADS_DEV + head) * KVW
                    place = (column * SPEC + position) * HEADS_DEV + head
                    store_lanes(
                        query_s,
                        pl.multiple_of(pair * 32 * ASK_STEP, 8),
                        place * ASK_STEP,
                        query_v[pair, position, :, at : at + KVW],
                    )
        return carry

    lax.fori_loop(0, 8, spread_queries, 0)

    replica = lax.axis_index("rep")
    rows = SPEC * HEADS
    late = iota2(rows, 1, 0) // HEADS_DEV % SPEC - SPEC + 1

    def attend(i, offset, length, window):
        held = [pick_ref[0, jnp.minimum(offset + j, PAGES_DEV - 1)] for j in range(window)]
        keys = load_lanes(
            key_s,
            [group * 8 * KEY_STEP + page for group in range(8) for page in held],
            KEY_STEP,
        )
        asked = load_lanes(
            query_s, [block * 8 * ASK_STEP + i for block in range(rows // 8)], ASK_STEP
        )
        scores = lax.dot_general(
            asked, keys, (((1,), (1,)), ((), ())), preferred_element_type=F32
        )
        span = window * 8
        key = iota2(1, 8 * span, 1)
        token = key % span // 8 * PAGE + key // span * 8 + key % 8
        scores = jnp.where(token < late + length, scores * SCORE_SCALE, -1e30)
        exponent = jnp.exp(scores - jnp.max(scores, axis=1, keepdims=True))
        total = jnp.sum(exponent, axis=1, keepdims=True)
        latent = mm(exponent.astype(BF), keys[:, :LAT]) / total
        out_ref[:, pl.ds(pl.multiple_of(i * 16, 16), 16), :] = latent.astype(BF).reshape(
            N_EP, 16, LAT
        )

    def request(i, offset):
        count = count_ref[replica, 0, i]
        length = (count - 1) * PAGE + fill_ref[replica, 0, i]
        for least, window in zip((0,) + WINDOWS, WINDOWS):
            pl.when((count > least) & (count <= window))(
                functools.partial(attend, i, offset, length, window)
            )
        result_copy(i).start()
        return offset + count

    lax.fori_loop(0, REQ_DEV, request, jnp.int32(0))
    for i in range(REQ_DEV):
        result_copy(i).wait()


def attention(page_order, page_count, last_fill, queries, pages):
    few = pl.BlockSpec(memory_space=pltpu.SMEM)
    far = pl.BlockSpec(memory_space=pltpu.HBM)
    return pl.pallas_call(
        attention_body,
        in_specs=[few, few, few, far, far],
        out_specs=far,
        out_shape=pltpu.HBM((N_EP, REQ_DEV * 16, LAT), BF),
        scratch_shapes=[
            pltpu.VMEM((LANES, PAGE * KEY_STEP, 128), F32),
            pltpu.VMEM((LANES, SPEC * HEADS * ASK_STEP, 128), F32),
            pltpu.VMEM((8, PAGES_DEV, SPAN), BF),
            pltpu.VMEM((8, SPEC, REQ_DEV, SPAN), BF),
            pltpu.VMEM((N_EP, REQ_DEV * 16, LAT), BF),
            pltpu.SemaphoreType.DMA((8,)),
            pltpu.SemaphoreType.DMA((8, SPEC)),
            pltpu.SemaphoreType.DMA((REQ_DEV,)),
        ],
        cost_estimate=pl.CostEstimate(
            flops=7 << 30, bytes_accessed=8 << 20, transcendentals=8 * 256 * 768
        ),
        compiler_params=pltpu.CompilerParams(vmem_limit_bytes=40 << 20),
        name="attention",
    )(*[distant(each) for each in (page_order, page_count, last_fill, queries, pages)])


def weight_loads(weight_hbm, weight_ref, sems):
    loads = []
    for band in range(4):
        columns = pl.ds(band * BAND, BAND)
        loads.append(
            pltpu.make_async_copy(
                weight_hbm.at[:, columns], weight_ref.at[:, columns], sems.at[band]
            )
        )
        loads[-1].start()
    return loads


def part_of(order_ref, lifted_ref, picked_ref, weight_ref, load, band, first):
    for place in range(8):
        source = order_ref[band * N_EP + first + place]
        picked_ref[place * 32 : place * 32 + 32, :] = lifted_ref[source]
    load.wait()
    return mm(picked_ref[...], weight_ref[:, band * BAND : (band + 1) * BAND]).astype(BF)


def sent_body(order_ref, latent_ref, up_hbm, weight_hbm, *rest):
    outs, lifted_ref = rest[:4], rest[4]
    split_ref, picked_ref, part_ref, up_ref, weight_ref, in_sems, sems = rest[5:]
    up_load = pltpu.make_async_copy(up_hbm, up_ref, in_sems.at[4])
    up_load.start()
    loads = weight_loads(weight_hbm, weight_ref, in_sems)
    by_head = rows_first(
        lambda r: (r // 32 % 2) * 128 + (r % 8) * 16 + (r // 8 % 4) * 4 + r // 64
    )

    def split(turn, carry):
        for part in range(4):
            step = turn * 4 + part
            both = mm(by_head, latent_ref[step]).astype(BF)
            at = pl.multiple_of(step * 64, 64)
            for head in range(HEADS_DEV):
                split_ref[head, pl.ds(at, 64), :] = both[head * 64 : head * 64 + 64]
        return carry

    lax.fori_loop(0, 2, split, 0)
    up_load.wait()
    for head in range(HEADS_DEV):
        lifted = mm(split_ref[head], up_ref[head]).astype(BF)
        columns = slice(head * VHEAD, (head + 1) * VHEAD)
        lifted_ref[:, :, columns] = lifted.reshape(N_EP, 32, VHEAD)
    copies = []
    for band in range(4):
        part_ref[band] = part_of(
            order_ref, lifted_ref, picked_ref, weight_ref, loads[band], band, 8
        )
        copies.append(pltpu.make_async_copy(part_ref.at[band], outs[band], sems.at[band]))
        copies[-1].start()
    for copy in copies:
        copy.wait()


def kept_body(order_ref, lifted_ref, weight_hbm, out_ref, picked_ref, weight_ref, in_sems):
    loads = weight_loads(weight_hbm, weight_ref, in_sems)
    for band in range(4):
        out_ref[band] = part_of(
            order_ref, lifted_ref, picked_ref, weight_ref, loads[band], band, 0
        )


def project(order, latent, value_up, out_weight):
    few = pl.BlockSpec(memory_space=pltpu.SMEM)
    whole = pl.BlockSpec(memory_space=pltpu.VMEM)
    far = pl.BlockSpec(memory_space=pltpu.HBM)
    *sent, lifted = pl.pallas_call(
        sent_body,
        in_specs=[few, whole, far, far],
        out_specs=[far] * 4 + [whole],
        out_shape=[pltpu.HBM((256, BAND), BF)] * 4 + [pltpu.VMEM((N_EP, 32, 512), BF)],
        scratch_shapes=[
            pltpu.VMEM((HEADS_DEV, 512, LAT), BF),
            pltpu.VMEM((256, 512), BF),
            pltpu.VMEM((4, 256, BAND), BF),
            pltpu.VMEM((HEADS_DEV, LAT, VHEAD), BF),
            pltpu.VMEM((512, D), BF),
            pltpu.SemaphoreType.DMA((5,)),
            pltpu.SemaphoreType.DMA((4,)),
        ],
        cost_estimate=pl.CostEstimate(
            flops=2 << 30, bytes_accessed=8 << 20, transcendentals=0
        ),
        compiler_params=pltpu.CompilerParams(vmem_limit_bytes=20 << 20),
        name="project_sent",
    )(order, near(latent), distant(value_up), distant(out_weight))
    kept = pl.pallas_call(
        kept_body,
        in_specs=[few, whole, far],
        out_specs=whole,
        out_shape=pltpu.VMEM((4, 256, BAND), BF),
        scratch_shapes=[
            pltpu.VMEM((256, 512), BF),
            pltpu.VMEM((512, D), BF),
            pltpu.SemaphoreType.DMA((4,)),
        ],
        cost_estimate=pl.CostEstimate(
            flops=1 << 30, bytes_accessed=6 << 20, transcendentals=0
        ),
        compiler_params=pltpu.CompilerParams(vmem_limit_bytes=12 << 20),
        name="project_kept",
    )(order, near(lifted), distant(out_weight))
    return *sent, kept


def add_body(spread, kept_ref, *rest):
    came, send, stay = rest[:4], rest[4:-1], rest[-1]
    for band in range(4):
        total = kept_ref[band].astype(F32) + came[band][...].astype(F32)
        rows = stay.shape[1]
        stay[band] = total[:rows]
        if spread:
            columns = slice(band % 2 * BAND, (band % 2 + 1) * BAND)
            for place in range(1, 4):
                send[band // 2 * 3 + place - 1][:, columns] = total[
                    place * rows : (place + 1) * rows
                ].astype(BF)
        else:
            send[band][...] = total[rows:].astype(BF)


def add_pieces(kept, came, spread):
    parts = 4 if spread else 2
    rows = kept.shape[1] // parts
    shape, count = ((rows, 2 * BAND), 6) if spread else ((rows, BAND), 4)
    whole = pl.BlockSpec(memory_space=pltpu.VMEM)
    outs = pl.pallas_call(
        functools.partial(add_body, spread),
        in_specs=[whole] * 5,
        out_specs=[whole] * (count + 1),
        out_shape=[jax.ShapeDtypeStruct(shape, BF)] * count
        + [jax.ShapeDtypeStruct((4, rows, BAND), F32)],
        cost_estimate=pl.CostEstimate(
            flops=8 * rows * D, bytes_accessed=8 * rows * D, transcendentals=0
        ),
        compiler_params=pltpu.CompilerParams(vmem_limit_bytes=4 << 20),
        name="add_pieces",
    )(near(kept), *[near(piece) for piece in came])
    return outs[:-1], outs[-1]


def finish_body(pick_ref, kept_ref, *rest):
    came, own_ref, offer_ref = rest[:6], rest[6], rest[7]
    for band in range(4):
        columns = slice(band % 2 * BAND, (band % 2 + 1) * BAND)
        total = kept_ref[band]
        for piece in came[band // 2 * 3 : band // 2 * 3 + 3]:
            total = total + piece[:, columns].astype(F32)
        total = total.astype(BF)
        own_ref[:, band * BAND : (band + 1) * BAND] = total
        offer_ref[:, band * BAND : (band + 1) * BAND] = mm(pick_ref[...], total).astype(BF)


def finish(pick, kept, came):
    whole = pl.BlockSpec(memory_space=pltpu.VMEM)
    return pl.pallas_call(
        finish_body,
        in_specs=[whole] * 8,
        out_specs=[whole] * 2,
        out_shape=[
            jax.ShapeDtypeStruct((TOK_DEV, D), BF),
            jax.ShapeDtypeStruct((2 * SPEC, D), BF),
        ],
        compiler_params=pltpu.CompilerParams(vmem_limit_bytes=4 << 20),
        cost_estimate=pl.CostEstimate(flops=4 << 20, bytes_accessed=1 << 20, transcendentals=0),
        name="finish",
    )(near(pick), near(kept), *[near(piece) for piece in came])


def expert_body(x_ref, in_ref, out_hbm, o_hbm, x_s, h_s, o_ref, out_ref, sems, out_sem):
    loads = [pltpu.make_async_copy(out_hbm.at[0], out_ref, out_sem.at[0])]
    loads[0].start()
    apart = rows_first(lambda r: (r % 128 // 4) * 8 + (r // 128) * 4 + r % 4)
    joined = rows_first(lambda r: (r // 4 % 2) * 128 + (r // 8) * 4 + r % 4)
    for step in range(4):
        block = mm(apart, x_ref[step * 256 : step * 256 + 256, :]).astype(BF)
        x_s[step * 128 : step * 128 + 128, :HALF] = block[:128]
        x_s[step * 128 : step * 128 + 128, HALF:] = block[128:]

    def inner(step, carry):
        columns = pl.ds(pl.multiple_of(step * 512, 512), 512)
        value = mm(x_s[...], in_ref[0, :, columns])
        h_s[:, columns] = (value / (1.0 + jnp.exp(-value))).astype(BF)
        return carry

    lax.fori_loop(0, 2, inner, 0)
    for load in loads:
        load.wait()
    copies = []
    for at in range(0, HALF, 256):
        halves = [
            mm(h_s[...], out_ref[:, first + at : first + at + 256]).astype(BF)
            for first in (0, HALF)
        ]
        for step in range(4):
            rows = slice(step * 128, step * 128 + 128)
            both = jnp.concatenate((halves[0][rows], halves[1][rows]), axis=0)
            o_ref[step * 256 : step * 256 + 256, at : at + 256] = mm(joined, both).astype(BF)
        copies.append(
            pltpu.make_async_copy(
                o_ref.at[:, pl.ds(at, 256)], o_hbm.at[:, pl.ds(at, 256)], sems.at[at // 256]
            )
        )
        copies[-1].start()
    for copy in copies:
        copy.wait()


def expert(incoming, expert_in, expert_out):
    whole = pl.BlockSpec(memory_space=pltpu.VMEM)
    far = pl.BlockSpec(memory_space=pltpu.HBM)
    return pl.pallas_call(
        expert_body,
        in_specs=[whole, whole, far],
        out_specs=far,
        out_shape=pltpu.HBM((DEVICES * 8, HALF), BF),
        scratch_shapes=[
            pltpu.VMEM((512, D), BF),
            pltpu.VMEM((512, FFE), BF),
            pltpu.VMEM((DEVICES * 8, HALF), BF),
            pltpu.VMEM((FFE, D), BF),
            pltpu.SemaphoreType.DMA((7,)),
            pltpu.SemaphoreType.DMA((4,)),
        ],
        cost_estimate=pl.CostEstimate(
            flops=8 << 30, bytes_accessed=22 << 20, transcendentals=512 * 1024
        ),
        compiler_params=pltpu.CompilerParams(vmem_limit_bytes=32 << 20),
        name="expert",
    )(near(incoming), near(expert_in), distant(expert_out))


NEAR = [(0, 1), (1, 0), (2, 3), (3, 2)]
FAR = [(0, 3), (3, 0), (1, 2), (2, 1)]
PAIRS = {1: NEAR, 3: FAR, 2: [(0, 2), (2, 0), (1, 3), (3, 1)]}
ROUTES = (
    (("ep_0", 1), ("ep_0", 3), ("ep_1", 1), ("ep_1", 3)),
    (("ep_0", 3), ("ep_0", 1), ("ep_1", 1), ("ep_1", 3)),
    (("ep_1", 1), ("ep_1", 3), ("ep_0", 1), ("ep_0", 3)),
    (("ep_1", 3), ("ep_1", 1), ("ep_0", 1), ("ep_0", 3)),
)


def block_order():
    first, second = [], []
    for route in ROUTES:
        places = [(0, 0)]
        for axis, flip in reversed(route):
            turn = (flip, 0) if axis == "ep_0" else (0, flip)
            places = places + [(a ^ turn[0], b ^ turn[1]) for a, b in places]
        first += [a for a, _ in places]
        second += [b for _, b in places]
    mine = lax.axis_index("ep_0"), lax.axis_index("ep_1")
    return (jnp.array(first, jnp.int32) ^ mine[0]) * 4 + (jnp.array(second, jnp.int32) ^ mine[1])


def exchange(pieces, step):
    out = []
    for band, piece in enumerate(pieces):
        axis, flip = ROUTES[band][step]
        out.append(lax.ppermute(piece, axis, PAIRS[flip]))
    return out


def sum_over_columns(pick, parts):
    *send, kept = parts
    for step in range(2):
        send, kept = add_pieces(kept, exchange(send, step), spread=step > 0)
    came = []
    for at, piece in enumerate(send):
        axis, third = ROUTES[at // 3 * 2][2]
        _, last = ROUTES[at // 3 * 2][3]
        flip = (last, third, third ^ last)[at % 3]
        came.append(lax.ppermute(piece, axis, PAIRS[flip]))
    return finish(pick, kept, came)


def shifted(value, axis, steps):
    count = lax.axis_size(axis)
    return lax.ppermute(value, axis, [(s, (s + steps) % count) for s in range(count)])


def from_replicas(value, odd):
    crossed = lax.ppermute(value, "rep", [(i, i ^ 1) for i in range(8)])
    value = jnp.where(odd, crossed, value)
    planes = [shifted(value, "rep", 2 * back) for back in range(1, 4)]
    return jnp.concatenate([value] + planes, axis=0)


def by_position(value):
    return jnp.concatenate([value[:, s * D : (s + 1) * D] for s in range(SPEC)], axis=0)


def by_slot(value):
    return jnp.concatenate([value[s * REQ_DEV : (s + 1) * REQ_DEV] for s in range(SPEC)], axis=1)


def per_device(
    latent_pages,
    queries,
    residual,
    page_count,
    last_fill,
    page_order,
    shed_slots,
    shed_shift,
    expert_ids,
    gate_weight,
    expert_home,
    norm_gain,
    value_up,
    out_weight,
    expert_in,
    expert_out,
):
    replica = lax.axis_index("rep")
    latent = attention(page_order, page_count, last_fill, queries, latent_pages)
    latent = lax.all_to_all(latent, EP, split_axis=0, concat_axis=0, tiled=True)
    tokens = jnp.arange(TOK_DEV, dtype=jnp.int32)
    own_sheds = shed_slots[replica, 0, :]
    shed_rows = (jnp.arange(SPEC, dtype=jnp.int32) * REQ_DEV + own_sheds[:, None]).reshape(-1)
    pick = shed_rows[:, None] == tokens[None, :]
    present = jnp.any(pick, axis=0)[:, None]
    row_shifts = jnp.repeat(shed_shift[0], SPEC)
    odd = (row_shifts % 2 == 1)[:, None]
    planes = (row_shifts + 1 - replica % 2) // 2 % 4
    wanted = jnp.arange(4, dtype=jnp.int32)[:, None] == planes[None, :]
    place = (wanted[:, :, None] & pick[None, :, :]).reshape(4 * 2 * SPEC, TOK_DEV).astype(BF)
    pick = pick.astype(BF)

    def served(own, came):
        taken = lax.dot_general(place, came, (((0,), (0,)), ((), ())), preferred_element_type=F32)
        return jnp.where(present, taken.astype(BF), own)

    own_residual = by_position(residual)
    came = from_replicas(mm(pick, own_residual).astype(BF), odd)
    latent, came = lax.optimization_barrier((latent, came))
    served_residual = served(own_residual, came)
    own_branch, offer = sum_over_columns(
        pick, project(block_order(), latent.reshape(8, 256, LAT), value_up, out_weight)
    )
    served_branch = served(own_branch, from_replicas(offer, odd))
    mixed = served_residual.astype(F32) + served_branch.astype(F32)
    square = jnp.mean(mixed * mixed, axis=1, keepdims=True)
    normed = (mixed * lax.rsqrt(square + NORM_EPS) * norm_gain).astype(BF)

    def routed(value):
        return value.reshape(REQ_DEV, SPEC, TOP).transpose(1, 0, 2).reshape(TOK_DEV, TOP)

    gate_weight = routed(gate_weight)
    target = expert_home[routed(expert_ids).reshape(-1)]
    hits = (target[:, None] == jnp.arange(DEVICES, dtype=jnp.int32)[None, :]).astype(jnp.int32)
    before = jnp.sum((jnp.cumsum(hits, axis=0) - hits) * hits, axis=1)
    slot = (target * CAP + before).reshape(TOK_DEV, TOP)
    row = jnp.arange(DEVICES * 8, dtype=jnp.int32)
    row_slot = row // 8 * CAP + row % CAP
    row_half = row // CAP % 2
    both = jnp.arange(2 * TOK_DEV, dtype=jnp.int32)
    same_half = row_half[None, :] == (both // TOK_DEV)[:, None]
    landing = slot[:, :, None] == row_slot[None, None, :]
    chosen = jnp.any(landing, axis=1)
    chooser = (jnp.concatenate((chosen, chosen)) & same_half).astype(BF)
    gates = jnp.sum(jnp.where(landing, gate_weight[:, :, None], 0.0), axis=1)
    gates = jnp.where(same_half, jnp.concatenate((gates, gates)), 0.0)
    coarse = lax.reduce_precision(gates, 8, 7)
    gates = jnp.concatenate((coarse.astype(BF), (gates - coarse).astype(BF)))

    def halves(value):
        return jnp.concatenate((value[:, :HALF], value[:, HALF:]), axis=0)

    outgoing = lax.dot_general(
        chooser, halves(normed), (((0,), (0,)), ((), ())), preferred_element_type=F32
    ).astype(BF)
    incoming = lax.all_to_all(outgoing, REP_EP, split_axis=0, concat_axis=0, tiled=True)
    outer = expert(incoming, expert_in, expert_out)
    returned = lax.all_to_all(outer, REP_EP, split_axis=0, concat_axis=0, tiled=True)
    moe = mm(gates, returned)
    layer = (halves(mixed) + moe[: 2 * TOK_DEV] + moe[2 * TOK_DEV :]).astype(BF)
    layer_out = jnp.concatenate((layer[:TOK_DEV], layer[TOK_DEV:]), axis=1)
    return by_slot(served_branch), by_slot(layer_out)


def solution(mesh):
    torus = Mesh(mesh.devices.reshape(mesh.shape["rep"], 4, 4), ("rep", "ep_0", "ep_1"))

    return jax.shard_map(
        per_device,
        mesh=torus,
        in_specs=(
            P(REP_EP, None),
            P(REP_EP, None),
            P(REP_EP, None),
            P(None, EP, None),
            P(None, EP, None),
            P(REP_EP, None),
            P(None, EP, None),
            P(EP, None),
            P(REP_EP, None),
            P(REP_EP, None),
            P(),
            P(),
            P(EP, None, None),
            P(EP, None),
            P(REP_EP, None, None),
            P(REP_EP, None, None),
        ),
        out_specs=(P(REP_EP, None), P(REP_EP, None)),
        check_vma=False,
    )
```
